32 devices in a mesh: lon: 8 (over y, x, core), dp: 4 (over z).
Axes of the slice: x: 2, y: 2, z: 4, core: 2. Of those that a mesh axis runs over, the one named last changes fastest.
Arguments:
- inputs: bfloat16 [4, 32, 384, 256], P('dp', None, 'lon'), may hold values from -6 to 6
- pre_act: bfloat16 [4, 32, 384, 256], P('dp', None, 'lon'), may hold values from -6 to 6
- cotangent: bfloat16 [4, 32, 384, 256], P('dp', None, 'lon'), may hold values from -6 to 6
- first_weight: bfloat16 [2304, 256], replicated, may hold values from -0.125 to 0.125
- second_weight: bfloat16 [2304, 256], replicated, may hold values from -0.125 to 0.125
Outputs:
- input_gradient_array: bfloat16 [4, 32, 384, 256], P('dp', None, 'lon')
- first_weight_gradient: float32 [589824], P(('lon', 'dp'))
- second_weight_gradient: float32 [589824], P(('lon', 'dp'))
The draws below stay inside these ranges and needn't reach their ends.
All inputs are finite; a program needn't handle non-finite values.
Results may differ from the reference program's by a relative error of at most 0.0049.
Values may be sent and summed in bfloat16 or wider, within the bound.
A program may use at most 64 MiB of HBM per device.

```python
import jax
import jax.numpy as jnp

C = 256
FIRST_SPREAD = 12
SECOND_SPREAD = 18
LAT = 32
NLON = 384
SAMPLES = 4


def shard_levels(stream_key, shape, split, least, largest):
    def one(axis_at, blocks):
        steps = jax.random.uniform(jax.random.fold_in(jax.random.fold_in(stream_key, 6), axis_at), (blocks,), jnp.float32, least / len(split), largest / len(split))
        return jnp.repeat(jnp.exp(steps), shape[axis_at] // blocks).reshape((-1,) + (1,) * (len(shape) - axis_at - 1))

    level = one(*split[0])
    for cut in split[1:]:
        level = level * one(*cut)
    return level


def bell_draw(key, extent, scale, bound, cuts=(), held_as=jnp.bfloat16):
    result = scale * jax.random.normal(key, extent, jnp.float32)
    if cuts:
        result = result * shard_levels(key, extent, cuts, -0.22, 0.18)
    return jnp.clip(result, -bound, bound).astype(held_as)


def setup_inputs(seed: int = 0) -> dict:
    seeds = jax.random.split(jax.random.key(seed), 6)
    return {
        "inputs": bell_draw(seeds[0], (SAMPLES, LAT, NLON, C), 1.0, 6.0, ((0, 4), (2, 8))),
        "pre_act": bell_draw(seeds[1], (SAMPLES, LAT, NLON, C), 1.0, 6.0, ((0, 4), (2, 8))),
        "cotangent": bell_draw(seeds[2], (SAMPLES, LAT, NLON, C), 1.0, 6.0, ((0, 4), (2, 8))),
        "first_weight": bell_draw(seeds[3], (9 * C, C), (9 * C) ** -0.5, 0.125),
        "second_weight": bell_draw(seeds[4], (9 * C, C), (9 * C) ** -0.5, 0.125),
    }


def lat_move(values, offset):
    rows = values.shape[1]
    if abs(offset) >= rows:
        return jnp.zeros_like(values)
    if offset == 0:
        return values
    blank = jnp.zeros_like(values[:, :abs(offset)])
    if offset > 0:
        return jnp.concatenate([values[:, offset:], blank], axis=1)
    return jnp.concatenate([blank, values[:, :rows + offset]], axis=1)


def shifted(values, dilation, tap, direction):
    lat_off = direction * (tap // 3 - 1) * dilation
    lon_off = direction * (tap % 3 - 1) * dilation
    return lat_move(jnp.roll(values, -lon_off, axis=2), lat_off)


def kernel_weight_gradient(source, dilation, upstream):
    chans = upstream.shape[3]
    flat_up = upstream.reshape(-1, chans)
    blocks = []
    for tap in range(9):
        moved = shifted(source, dilation, tap, 1).reshape(-1, source.shape[3])
        blocks.append(jnp.dot(moved.T, flat_up, preferred_element_type=jnp.float32))
    return jnp.concatenate(blocks, axis=0)


def gradient_wrt_input(upstream, dilation, weights):
    chans = weights.shape[1]
    total = jnp.zeros((upstream.shape[0] * upstream.shape[1] * upstream.shape[2], weights.shape[1]), jnp.float32)
    for tap in range(9):
        moved = shifted(upstream, dilation, tap, -1).reshape(-1, chans)
        block = weights[tap * chans:(tap + 1) * chans]
        total = total + jnp.dot(moved, block.T, preferred_element_type=jnp.float32)
    return total.reshape(upstream.shape)


def reference(inputs, pre_act, cotangent, first_weight, second_weight):
    norm_factor = float(SAMPLES * LAT * NLON) ** -0.5
    hidden_activation = jnp.maximum(pre_act, jnp.zeros_like(pre_act))
    second_weight_gradient = (kernel_weight_gradient(hidden_activation, SECOND_SPREAD, cotangent) * norm_factor).reshape(-1)
    hidden_gradient = gradient_wrt_input(cotangent, SECOND_SPREAD, second_weight)
    partial_gradient = jnp.where(pre_act > 0, hidden_gradient, jnp.float32(0.0)).astype(jnp.bfloat16)
    first_weight_gradient = (kernel_weight_gradient(inputs, FIRST_SPREAD, partial_gradient) * norm_factor).reshape(-1)
    input_gradient_array = gradient_wrt_input(partial_gradient, FIRST_SPREAD, first_weight).astype(jnp.bfloat16)
    return input_gradient_array, first_weight_gradient, second_weight_gradient
```

```python
import functools

import jax
import jax.numpy as jnp
from jax import lax
from jax.experimental import pallas as pl
from jax.experimental.pallas import tpu as pltpu
from jax.sharding import PartitionSpec as P

FIRST_SPREAD = 12
SECOND_SPREAD = 18
MESH = pl.DeviceIdType.MESH
F32 = jnp.float32
BF16 = jnp.bfloat16
LANE_SLOT = (0, 2, 1)


def row_span(rows, dilation, r):
    if r == 0:
        return 0, rows - dilation, dilation
    if r == 1:
        return 0, rows, 0
    return dilation, rows, 0


def dot_nt(a, b):
    return lax.dot_general(a, b, (((1,), (1,)), ((), ())), preferred_element_type=F32)


def dot_tn(a, b):
    return lax.dot_general(a, b, (((0,), (0,)), ((), ())), preferred_element_type=F32)


def flat(v):
    return v.reshape(-1, v.shape[-1])


def kernel(nl, nd, scatter, norm, *refs):
    inp, pre, cot, w1, w2 = refs[:5]
    ig_out, g1_out, g2_out = refs[5:8]
    (cot_v, pre_v, inp_v, lg_v, w1_v, w2_v, side2, side1, acc) = refs[8:17]
    (in_sem, w1_sem, w2_sem) = refs[17:20]
    (s2_lo, s2_hi, r2_lo, r2_hi, s1_lo, s1_hi, r1_lo, r1_hi, hs_sem, hr_sem) = refs[20:30]
    if scatter:
        (dw1, dw2, ps1, ps2, pr1, pr2, as1, as2, ar1, ar2) = refs[30:40]
        (zs1, zs2, zr1, zr2, p_ssem, p_rsem, a_ssem, a_rsem, z_ssem, z_rsem) = refs[40:50]
    else:
        dw1, dw2 = g1_out, g2_out

    rows, cols, ch = cot_v.shape
    me_l, me_d = lax.axis_index("lon"), lax.axis_index("dp")
    left, right = lax.rem(me_l + nl - 1, nl), lax.rem(me_l + 1, nl)
    half = nl // 2
    slots = half * nd
    core = lax.rem(me_l, 2)

    my_chip = me_l // 2

    def plane_device(t):
        return (2 * lax.rem(my_chip + t, half) + core, me_d)

    def depth_device(u):
        return (me_l, lax.rem(me_d + u, nd))

    load_cot = pltpu.make_async_copy(cot.at[0], cot_v, in_sem.at[0])
    load_pre = pltpu.make_async_copy(pre.at[0], pre_v, in_sem.at[1])
    load_inp = pltpu.make_async_copy(inp.at[0], inp_v, in_sem.at[2])

    def weight_loads(w, w_v, sem):
        return [
            pltpu.make_async_copy(
                w.at[pl.ds(k * ch, ch)],
                w_v.at[k // 3, :, pl.ds(LANE_SLOT.index(k % 3) * ch, ch)],
                sem.at[k],
            )
            for k in range(9)
        ]

    load_w2 = weight_loads(w2, w2_v, w2_sem)
    load_w1 = weight_loads(w1, w1_v, w1_sem)
    load_cot.start()
    for c in load_w2:
        c.start()
    load_pre.start()
    load_inp.start()
    for c in load_w1:
        c.start()

    barrier = pltpu.get_barrier_semaphore()
    for other in (left, right):
        pl.semaphore_signal(barrier, inc=1, device_id=(other, me_d), device_id_type=MESH)
    greeted = 2
    if scatter:
        for t in range(1, half):
            pl.semaphore_signal(barrier, inc=1, device_id=plane_device(t), device_id_type=MESH)
        for u in range(1, nd):
            pl.semaphore_signal(barrier, inc=1, device_id=depth_device(u), device_id_type=MESH)
        greeted += half - 1 + nd - 1

    def halo_copies(lo, hi, from_right, from_left, base):
        return (
            pltpu.make_async_remote_copy(
                src_ref=lo, dst_ref=from_right, send_sem=hs_sem.at[base],
                recv_sem=hr_sem.at[base], device_id=(left, me_d), device_id_type=MESH,
            ),
            pltpu.make_async_remote_copy(
                src_ref=hi, dst_ref=from_left, send_sem=hs_sem.at[base + 1],
                recv_sem=hr_sem.at[base + 1], device_id=(right, me_d), device_id_type=MESH,
            ),
        )

    def pack(src, lo, hi, d):
        for p in range(rows):
            lo[p * d : (p + 1) * d, :] = src[p, 0:d, :]
            hi[p * d : (p + 1) * d, :] = src[p, cols - d : cols, :]

    def side_inner(src, side, d):
        side[:, 0 : cols - d, 0:ch] = src[:, d:cols, :]
        side[:, d:cols, ch : 2 * ch] = src[:, 0 : cols - d, :]

    def side_edges(side, from_right, from_left, d):
        side[:, cols - d : cols, 0:ch] = from_right[...].reshape(rows, d, ch)
        side[:, 0:d, ch : 2 * ch] = from_left[...].reshape(rows, d, ch)

    def input_terms(src, lanes, w_v, wl, d, fresh):
        for r in (1, 0, 2):
            lo, hi, first = row_span(rows, d, r)
            term = dot_nt(
                flat(src[first : first + hi - lo, :, 0:lanes]), w_v[r, :, wl : wl + lanes]
            )
            if fresh and r == 1:
                acc[...] = term
            else:
                acc[lo * cols : hi * cols, :] += term

    def weight_terms(x, src, lanes, dw, taps, d):
        for r in range(3):
            lo, hi, first = row_span(rows, d, r)
            term = dot_tn(flat(x[lo:hi]), flat(src[first : first + hi - lo, :, 0:lanes]))
            for at, c in enumerate(taps):
                k = 3 * r + c
                value = term[:, at * ch : (at + 1) * ch]
                dw[k * ch : (k + 1) * ch, :] = value if scatter else value * norm

    if scatter:
        depth = dw1.shape[0] // (nl * nd)
        plane_order = (*range(1, half), 0)

        def chunk_rows(slot, parity):
            l, d = 2 * (slot // nd) + parity, lax.rem(slot, nd)
            return pl.ds(pl.multiple_of((l * nd + d) * depth, 8), depth)

        def pair_copy(ps, pr, at, t):
            part = pl.ds(lax.rem(my_chip + t, half) * nd, nd)
            return pltpu.make_async_remote_copy(
                src_ref=ps.at[part], dst_ref=pr.at[part],
                send_sem=p_ssem.at[at, t], recv_sem=p_rsem.at[at, t],
                device_id=(me_l + 1 - 2 * core, me_d), device_id_type=MESH,
            )

        def pair_send(dw, ps, pr, at):
            for t in plane_order:
                for d in range(nd):
                    s = lax.rem(my_chip + t, half) * nd + d
                    v = dw[chunk_rows(s, 1 - core), :].astype(BF16)
                    ps[s, 0:depth, :] = v[:, : ch // 2]
                    ps[s, depth : 2 * depth, :] = v[:, ch // 2 :]
                pair_copy(ps, pr, at, t).start()

        def chip_sum(dw, pr, s):
            v = dw[chunk_rows(s, core), :]
            return (
                v[:, : ch // 2] + pr[s, 0:depth, :].astype(F32),
                v[:, ch // 2 :] + pr[s, depth : 2 * depth, :].astype(F32),
            )

        def plane_copy(a_s, a_r, at, t):
            chip = lax.rem(my_chip + t, half)
            return pltpu.make_async_remote_copy(
                src_ref=a_s.at[pl.ds(chip * nd, nd)], dst_ref=a_r.at[pl.ds(t * nd, nd)],
                send_sem=a_ssem.at[at, t], recv_sem=a_rsem.at[at, t],
                device_id=plane_device(t), device_id_type=MESH,
            )

        def depth_copy(z_s, z_r, at, u):
            return pltpu.make_async_remote_copy(
                src_ref=z_s.at[lax.rem(me_d + u, nd)], dst_ref=z_r.at[u],
                send_sem=z_ssem.at[at, u], recv_sem=z_rsem.at[at, u],
                device_id=depth_device(u), device_id_type=MESH,
            )

        def spread(dw, ps, pr, a_s, a_r, at):
            for t in plane_order:
                pair_copy(ps, pr, at, t).wait()
                if t == 0:
                    continue
                for d in range(nd):
                    s = lax.rem(my_chip + t, half) * nd + d
                    lo, hi = chip_sum(dw, pr, s)
                    a_s[s, 0:depth, :] = lo.astype(BF16)
                    a_s[s, depth : 2 * depth, :] = hi.astype(BF16)
                plane_copy(a_s, a_r, at, t).start()

        def plane_sum(dw, pr, a_r, d):
            lo, hi = chip_sum(dw, pr, my_chip * nd + d)
            for t in range(1, half):
                lo += a_r[t * nd + d, 0:depth, :].astype(F32)
                hi += a_r[t * nd + d, depth : 2 * depth, :].astype(F32)
            return lo, hi

        def across(dw, pr, a_s, a_r, z_s, z_r, at):
            for t in range(1, half):
                plane_copy(a_s, a_r, at, t).wait()

            for u in range(1, nd):
                d = lax.rem(me_d + u, nd)
                lo, hi = plane_sum(dw, pr, a_r, d)
                z_s[d, 0:depth, :] = lo.astype(BF16)
                z_s[d, depth : 2 * depth, :] = hi.astype(BF16)
                depth_copy(z_s, z_r, at, u).start()

        def gather_sum(dw, pr, a_r, z_s, z_r, at, out):
            lo, hi = plane_sum(dw, pr, a_r, me_d)
            for u in range(1, nd):
                depth_copy(z_s, z_r, at, u).wait()
                lo += z_r[u, 0:depth, :].astype(F32)
                hi += z_r[u, depth : 2 * depth, :].astype(F32)
            out[pl.ds(0, depth, stride=2), :] = lo * norm
            out[pl.ds(1, depth, stride=2), :] = hi * norm

    load_cot.wait()
    pack(cot_v, s2_lo, s2_hi, SECOND_SPREAD)
    pl.semaphore_wait(barrier, greeted)
    halo2 = halo_copies(s2_lo, s2_hi, r2_lo, r2_hi, 0)
    for c in halo2:
        c.start()
    side_inner(cot_v, side2, SECOND_SPREAD)
    for c in load_w2:
        c.wait()
    input_terms(cot_v, ch, w2_v, 2 * ch, SECOND_SPREAD, True)
    load_pre.wait()
    zero = jnp.zeros((), BF16)
    pre_v[...] = jnp.maximum(pre_v[...], zero)
    weight_terms(pre_v, cot_v, ch, dw2, (1,), SECOND_SPREAD)
    for c in halo2:
        c.wait()
    side_edges(side2, r2_lo, r2_hi, SECOND_SPREAD)
    input_terms(side2, 2 * ch, w2_v, 0, SECOND_SPREAD, False)
    grad = jnp.where(flat(pre_v[...]) > 0, acc[...], F32(0.0)).astype(BF16)
    lg_v[...] = grad.reshape(rows, cols, ch)
    pack(lg_v, s1_lo, s1_hi, FIRST_SPREAD)
    halo1 = halo_copies(s1_lo, s1_hi, r1_lo, r1_hi, 2)
    for c in halo1:
        c.start()
    weight_terms(pre_v, side2, 2 * ch, dw2, (0, 2), SECOND_SPREAD)
    if scatter:
        pair_send(dw2, ps2, pr2, 0)

    load_inp.wait()
    side_inner(lg_v, side1, FIRST_SPREAD)
    weight_terms(inp_v, lg_v, ch, dw1, (1,), FIRST_SPREAD)
    if scatter:
        spread(dw2, ps2, pr2, as2, ar2, 0)
    for c in halo1:
        c.wait()
    side_edges(side1, r1_lo, r1_hi, FIRST_SPREAD)
    weight_terms(inp_v, side1, 2 * ch, dw1, (0, 2), FIRST_SPREAD)
    if scatter:
        pair_send(dw1, ps1, pr1, 1)
    for c in load_w1:
        c.wait()
    input_terms(lg_v, ch, w1_v, 2 * ch, FIRST_SPREAD, True)
    if scatter:
        spread(dw1, ps1, pr1, as1, ar1, 1)
        across(dw2, pr2, as2, ar2, zs2, zr2, 0)
    input_terms(side1, 2 * ch, w1_v, 0, FIRST_SPREAD, False)
    ig_out[0] = acc[...].astype(BF16).reshape(rows, cols, ch)
    if scatter:
        across(dw1, pr1, as1, ar1, zs1, zr1, 1)
        gather_sum(dw2, pr2, ar2, zs2, zr2, 0, g2_out)
        gather_sum(dw1, pr1, ar1, zs1, zr1, 1, g1_out)


def emit_kernel(*refs):
    count = len(refs) // 2
    copies = [
        pltpu.make_async_copy(refs[i], refs[count + i], refs[-1].at[i]) for i in range(count)
    ]
    for c in copies:
        c.start()
    for c in copies:
        c.wait()


def emit(*values):
    any_spec = pl.BlockSpec(memory_space=pl.ANY)
    vmem_spec = pl.BlockSpec(memory_space=pltpu.VMEM)
    return pl.pallas_call(
        emit_kernel,
        out_shape=[jax.ShapeDtypeStruct(v.shape, v.dtype) for v in values],
        in_specs=[vmem_spec] * len(values),
        out_specs=[any_spec] * len(values),
        scratch_shapes=[pltpu.SemaphoreType.DMA((len(values),))],
        name="emit",
    )(*(pltpu.with_memory_space_constraint(v, pltpu.VMEM) for v in values))


def local(nl, nd, inputs, pre_act, cotangent, first_weight, second_weight):
    _, rows, cols, ch = inputs.shape
    taps_rows = first_weight.shape[0]
    norm = float(rows * cols * nl * inputs.shape[0] * nd) ** -0.5
    devices = nl * nd
    depth = taps_rows // devices
    scatter = nl % 2 == 0 and taps_rows % devices == 0 and depth % 8 == 0
    slots = devices // 2
    vm = pltpu.VMEM
    dma = pltpu.SemaphoreType.DMA
    field = vm((rows, cols, ch), BF16)
    edge2 = vm((rows * SECOND_SPREAD, ch), BF16)
    edge1 = vm((rows * FIRST_SPREAD, ch), BF16)
    weights = vm((3, ch, 3 * ch), BF16)
    side = vm((rows, cols, 2 * ch), BF16)
    scratch = [field] * 4 + [weights] * 2 + [side] * 2 + [vm((rows * cols, ch), F32)]
    scratch += [dma((3,)), dma((9,)), dma((9,))]
    scratch += [edge2] * 4 + [edge1] * 4 + [dma((4,)), dma((4,))]
    if scatter:
        pieces = vm((slots, 2 * depth, ch // 2), BF16)
        scratch += [vm((taps_rows, ch), F32)] * 2 + [pieces] * 8
        scratch += [vm((nd, 2 * depth, ch // 2), BF16)] * 4
        scratch += [dma((2, nl // 2))] * 4 + [dma((2, nd))] * 2
        grad_shape = (2 * depth, ch // 2)
    else:
        grad_shape = (taps_rows, ch)
    any_spec = pl.BlockSpec(memory_space=pl.ANY)
    vmem_spec = pl.BlockSpec(memory_space=pltpu.VMEM)
    place = vm if scatter else jax.ShapeDtypeStruct
    ig, g1, g2 = pl.pallas_call(
        functools.partial(kernel, nl, nd, scatter, norm),
        out_shape=(
            place(inputs.shape, BF16),
            place(grad_shape, F32),
            place(grad_shape, F32),
        ),
        in_specs=[any_spec] * 5,
        out_specs=(vmem_spec, vmem_spec, vmem_spec),
        scratch_shapes=scratch,
        compiler_params=pltpu.CompilerParams(
            collective_id=0, has_side_effects=True, vmem_limit_bytes=48 * 1024 * 1024
        ),
        name="conv_backward",
    )(inputs, pre_act, cotangent, first_weight, second_weight)
    if scatter:
        ig, g1, g2 = emit(ig, g1, g2)
    g1, g2 = g1.reshape(-1), g2.reshape(-1)
    if not scatter:
        g1, g2 = (lax.psum_scatter(g, "lon", scatter_dimension=0, tiled=True) for g in (g1, g2))
        g1, g2 = (lax.psum_scatter(g, "dp", scatter_dimension=0, tiled=True) for g in (g1, g2))
    return ig, g1, g2


def solution(mesh):
    in_specs = (
        P("dp", None, "lon", None),
        P("dp", None, "lon", None),
        P("dp", None, "lon", None),
        P(),
        P(),
    )
    out_specs = (P("dp", None, "lon", None), P(("lon", "dp")), P(("lon", "dp")))
    step = functools.partial(local, mesh.shape["lon"], mesh.shape["dp"])
    return jax.shard_map(step, mesh=mesh, in_specs=in_specs, out_specs=out_specs, check_vma=False)
```

```python
import functools

import jax
import jax.numpy as jnp
from jax import lax
from jax.experimental import pallas as pl
from jax.experimental.pallas import tpu as pltpu
from jax.sharding import PartitionSpec as P

FIRST_SPREAD = 12
SECOND_SPREAD = 18
MESH = pl.DeviceIdType.MESH
F32 = jnp.float32
BF16 = jnp.bfloat16
LANE_SLOT = (0, 2, 1)


def row_span(rows, dilation, r):
    if r == 0:
        return 0, rows - dilation, dilation
    if r == 1:
        return 0, rows, 0
    return dilation, rows, 0


def dot_nt(a, b):
    return lax.dot_general(a, b, (((1,), (1,)), ((), ())), preferred_element_type=F32)


def dot_tn(a, b):
    return lax.dot_general(a, b, (((0,), (0,)), ((), ())), preferred_element_type=F32)


def flat(v):
    return v.reshape(-1, v.shape[-1])


def kernel(nl, nd, scatter, norm, *refs):
    inp, pre, cot, w1, w2 = refs[:5]
    ig_out, g1_out, g2_out = refs[5:8]
    (cot_v, pre_v, inp_v, lg_v, w1_v, w2_v, side2, side1, acc) = refs[8:17]
    (in_sem, w1_sem, w2_sem) = refs[17:20]
    (s2_lo, s2_hi, r2_lo, r2_hi, s1_lo, s1_hi, r1_lo, r1_hi, hs_sem, hr_sem) = refs[20:30]
    if scatter:
        (dw1, dw2, ps1, ps2, pr1, pr2, as1, as2, ar1, ar2) = refs[30:40]
        (zs1, zs2, zr1, zr2, p_ssem, p_rsem, a_ssem, a_rsem, z_ssem, z_rsem) = refs[40:50]
    else:
        dw1, dw2 = g1_out, g2_out

    rows, cols, ch = cot_v.shape
    me_l, me_d = lax.axis_index("lon"), lax.axis_index("dp")
    left, right = lax.rem(me_l + nl - 1, nl), lax.rem(me_l + 1, nl)
    half = nl // 2
    slots = half * nd
    core = lax.rem(me_l, 2)

    my_chip = me_l // 2

    def plane_device(t):
        return (2 * lax.rem(my_chip + t, half) + core, me_d)

    def depth_device(u):
        return (me_l, lax.rem(me_d + u, nd))

    load_cot = pltpu.make_async_copy(cot.at[0], cot_v, in_sem.at[0])
    load_pre = pltpu.make_async_copy(pre.at[0], pre_v, in_sem.at[1])
    load_inp = pltpu.make_async_copy(inp.at[0], inp_v, in_sem.at[2])

    def weight_loads(w, w_v, sem):
        return [
            pltpu.make_async_copy(
                w.at[pl.ds(k * ch, ch)],
                w_v.at[k // 3, :, pl.ds(LANE_SLOT.index(k % 3) * ch, ch)],
                sem.at[k],
            )
            for k in range(9)
        ]

    load_w2 = weight_loads(w2, w2_v, w2_sem)
    load_w1 = weight_loads(w1, w1_v, w1_sem)
    load_cot.start()
    for c in load_w2:
        c.start()
    load_pre.start()
    load_inp.start()
    for c in load_w1:
        c.start()

    barrier = pltpu.get_barrier_semaphore()
    for other in (left, right):
        pl.semaphore_signal(barrier, inc=1, device_id=(other, me_d), device_id_type=MESH)
    greeted = 2
    if scatter:
        for t in range(1, half):
            pl.semaphore_signal(barrier, inc=1, device_id=plane_device(t), device_id_type=MESH)
        for u in range(1, nd):
            pl.semaphore_signal(barrier, inc=1, device_id=depth_device(u), device_id_type=MESH)
        greeted += half - 1 + nd - 1

    def halo_copies(lo, hi, from_right, from_left, base):
        return (
            pltpu.make_async_remote_copy(
                src_ref=lo, dst_ref=from_right, send_sem=hs_sem.at[base],
                recv_sem=hr_sem.at[base], device_id=(left, me_d), device_id_type=MESH,
            ),
            pltpu.make_async_remote_copy(
                src_ref=hi, dst_ref=from_left, send_sem=hs_sem.at[base + 1],
                recv_sem=hr_sem.at[base + 1], device_id=(right, me_d), device_id_type=MESH,
            ),
        )

    def pack(src, lo, hi, d):
        for p in range(rows):
            lo[p * d : (p + 1) * d, :] = src[p, 0:d, :]
            hi[p * d : (p + 1) * d, :] = src[p, cols - d : cols, :]

    def side_inner(src, side, d):
        side[:, 0 : cols - d, 0:ch] = src[:, d:cols, :]
        side[:, d:cols, ch : 2 * ch] = src[:, 0 : cols - d, :]

    def side_edges(side, from_right, from_left, d):
        side[:, cols - d : cols, 0:ch] = from_right[...].reshape(rows, d, ch)
        side[:, 0:d, ch : 2 * ch] = from_left[...].reshape(rows, d, ch)

    def input_terms(src, lanes, w_v, wl, d, fresh):
        for r in (1, 0, 2):
            lo, hi, first = row_span(rows, d, r)
            term = dot_nt(
                flat(src[first : first + hi - lo, :, 0:lanes]), w_v[r, :, wl : wl + lanes]
            )
            if fresh and r == 1:
                acc[...] = term
            else:
                acc[lo * cols : hi * cols, :] += term

    def weight_terms(x, src, lanes, dw, taps, d):
        for r in range(3):
            lo, hi, first = row_span(rows, d, r)
            term = dot_tn(flat(x[lo:hi]), flat(src[first : first + hi - lo, :, 0:lanes]))
            for at, c in enumerate(taps):
                k = 3 * r + c
                value = term[:, at * ch : (at + 1) * ch]
                dw[k * ch : (k + 1) * ch, :] = value if scatter else value * norm

    if scatter:
        depth = dw1.shape[0] // (nl * nd)
        plane_order = (*range(1, half), 0)

        def chunk_rows(slot, parity):
            l, d = 2 * (slot // nd) + parity, lax.rem(slot, nd)
            return pl.ds(pl.multiple_of((l * nd + d) * depth, 8), depth)

        def pair_copy(ps, pr, at, t):
            part = pl.ds(lax.rem(my_chip + t, half) * nd, nd)
            return pltpu.make_async_remote_copy(
                src_ref=ps.at[part], dst_ref=pr.at[part],
                send_sem=p_ssem.at[at, t], recv_sem=p_rsem.at[at, t],
                device_id=(me_l + 1 - 2 * core, me_d), device_id_type=MESH,
            )

        def pair_send(dw, ps, pr, at):
            for t in plane_order:
                for d in range(nd):
                    s = lax.rem(my_chip + t, half) * nd + d
                    v = dw[chunk_rows(s, 1 - core), :].astype(BF16)
                    ps[s, 0:depth, :] = v[:, : ch // 2]
                    ps[s, depth : 2 * depth, :] = v[:, ch // 2 :]
                pair_copy(ps, pr, at, t).start()

        def chip_sum(dw, pr, s):
            v = dw[chunk_rows(s, core), :]
            return (
                v[:, : ch // 2] + pr[s, 0:depth, :].astype(F32),
                v[:, ch // 2 :] + pr[s, depth : 2 * depth, :].astype(F32),
            )

        def plane_copy(a_s, a_r, at, t):
            chip = lax.rem(my_chip + t, half)
            return pltpu.make_async_remote_copy(
                src_ref=a_s.at[pl.ds(chip * nd, nd)], dst_ref=a_r.at[pl.ds(t * nd, nd)],
                send_sem=a_ssem.at[at, t], recv_sem=a_rsem.at[at, t],
                device_id=plane_device(t), device_id_type=MESH,
            )

        def depth_copy(z_s, z_r, at, u):
            return pltpu.make_async_remote_copy(
                src_ref=z_s.at[lax.rem(me_d + u, nd)], dst_ref=z_r.at[u],
                send_sem=z_ssem.at[at, u], recv_sem=z_rsem.at[at, u],
                device_id=depth_device(u), device_id_type=MESH,
            )

        def spread(dw, ps, pr, a_s, a_r, at):
            for t in plane_order:
                pair_copy(ps, pr, at, t).wait()
                if t == 0:
                    continue
                for d in range(nd):
                    s = lax.rem(my_chip + t, half) * nd + d
                    lo, hi = chip_sum(dw, pr, s)
                    a_s[s, 0:depth, :] = lo.astype(BF16)
                    a_s[s, depth : 2 * depth, :] = hi.astype(BF16)
                plane_copy(a_s, a_r, at, t).start()

        def plane_sum(dw, pr, a_r, d):
            lo, hi = chip_sum(dw, pr, my_chip * nd + d)
            for t in range(1, half):
                lo += a_r[t * nd + d, 0:depth, :].astype(F32)
                hi += a_r[t * nd + d, depth : 2 * depth, :].astype(F32)
            return lo, hi

        def across(dw, pr, a_s, a_r, z_s, z_r, at):
            for t in range(1, half):
                plane_copy(a_s, a_r, at, t).wait()

            for u in range(1, nd):
                d = lax.rem(me_d + u, nd)
                lo, hi = plane_sum(dw, pr, a_r, d)
                z_s[d, 0:depth, :] = lo.astype(BF16)
                z_s[d, depth : 2 * depth, :] = hi.astype(BF16)
                depth_copy(z_s, z_r, at, u).start()

        def gather_sum(dw, pr, a_r, z_s, z_r, at, out):
            lo, hi = plane_sum(dw, pr, a_r, me_d)
            for u in range(1, nd):
                depth_copy(z_s, z_r, at, u).wait()
                lo += z_r[u, 0:depth, :].astype(F32)
                hi += z_r[u, depth : 2 * depth, :].astype(F32)
            out[pl.ds(0, depth, stride=2), :] = lo * norm
            out[pl.ds(1, depth, stride=2), :] = hi * norm

    load_cot.wait()
    pack(cot_v, s2_lo, s2_hi, SECOND_SPREAD)
    pl.semaphore_wait(barrier, greeted)
    halo2 = halo_copies(s2_lo, s2_hi, r2_lo, r2_hi, 0)
    for c in halo2:
        c.start()
    side_inner(cot_v, side2, SECOND_SPREAD)
    for c in load_w2:
        c.wait()
    input_terms(cot_v, ch, w2_v, 2 * ch, SECOND_SPREAD, True)
    load_pre.wait()
    zero = jnp.zeros((), BF16)
    pre_v[...] = jnp.maximum(pre_v[...], zero)
    weight_terms(pre_v, cot_v, ch, dw2, (1,), SECOND_SPREAD)
    for c in halo2:
        c.wait()
    side_edges(side2, r2_lo, r2_hi, SECOND_SPREAD)
    input_terms(side2, 2 * ch, w2_v, 0, SECOND_SPREAD, False)
    grad = jnp.where(flat(pre_v[...]) > 0, acc[...], F32(0.0)).astype(BF16)
    lg_v[...] = grad.reshape(rows, cols, ch)
    pack(lg_v, s1_lo, s1_hi, FIRST_SPREAD)
    halo1 = halo_copies(s1_lo, s1_hi, r1_lo, r1_hi, 2)
    for c in halo1:
        c.start()
    weight_terms(pre_v, side2, 2 * ch, dw2, (0, 2), SECOND_SPREAD)
    if scatter:
        pair_send(dw2, ps2, pr2, 0)

    load_inp.wait()
    side_inner(lg_v, side1, FIRST_SPREAD)
    weight_terms(inp_v, lg_v, ch, dw1, (1,), FIRST_SPREAD)
    if scatter:
        spread(dw2, ps2, pr2, as2, ar2, 0)
    for c in halo1:
        c.wait()
    side_edges(side1, r1_lo, r1_hi, FIRST_SPREAD)
    weight_terms(inp_v, side1, 2 * ch, dw1, (0, 2), FIRST_SPREAD)
    if scatter:
        pair_send(dw1, ps1, pr1, 1)
    for c in load_w1:
        c.wait()
    input_terms(lg_v, ch, w1_v, 2 * ch, FIRST_SPREAD, True)
    if scatter:
        spread(dw1, ps1, pr1, as1, ar1, 1)
        across(dw2, pr2, as2, ar2, zs2, zr2, 0)
    input_terms(side1, 2 * ch, w1_v, 0, FIRST_SPREAD, False)
    ig_out[0] = acc[...].astype(BF16).reshape(rows, cols, ch)
    if scatter:
        across(dw1, pr1, as1, ar1, zs1, zr1, 1)
        gather_sum(dw2, pr2, ar2, zs2, zr2, 0, g2_out)
        gather_sum(dw1, pr1, ar1, zs1, zr1, 1, g1_out)


def emit_kernel(*refs):
    count = len(refs) // 2
    copies = [
        pltpu.make_async_copy(refs[i], refs[count + i], refs[-1].at[i]) for i in range(count)
    ]
    for c in copies:
        c.start()
    for c in copies:
        c.wait()


def emit(*values):
    any_spec = pl.BlockSpec(memory_space=pl.ANY)
    vmem_spec = pl.BlockSpec(memory_space=pltpu.VMEM)
    return pl.pallas_call(
        emit_kernel,
        out_shape=[jax.ShapeDtypeStruct(v.shape, v.dtype) for v in values],
        in_specs=[vmem_spec] * len(values),
        out_specs=[any_spec] * len(values),
        scratch_shapes=[pltpu.SemaphoreType.DMA((len(values),))],
        name="emit",
    )(*(pltpu.with_memory_space_constraint(v, pltpu.VMEM) for v in values))


def local(nl, nd, inputs, pre_act, cotangent, first_weight, second_weight):
    _, rows, cols, ch = inputs.shape
    taps_rows = first_weight.shape[0]
    norm = float(rows * cols * nl * inputs.shape[0] * nd) ** -0.5
    devices = nl * nd
    depth = taps_rows // devices
    scatter = nl % 2 == 0 and taps_rows % devices == 0 and depth % 8 == 0
    slots = devices // 2
    vm = pltpu.VMEM
    dma = pltpu.SemaphoreType.DMA
    field = vm((rows, cols, ch), BF16)
    edge2 = vm((rows * SECOND_SPREAD, ch), BF16)
    edge1 = vm((rows * FIRST_SPREAD, ch), BF16)
    weights = vm((3, ch, 3 * ch), BF16)
    side = vm((rows, cols, 2 * ch), BF16)
    scratch = [field] * 4 + [weights] * 2 + [side] * 2 + [vm((rows * cols, ch), F32)]
    scratch += [dma((3,)), dma((9,)), dma((9,))]
    scratch += [edge2] * 4 + [edge1] * 4 + [dma((4,)), dma((4,))]
    if scatter:
        pieces = vm((slots, 2 * depth, ch // 2), BF16)
        scratch += [vm((taps_rows, ch), F32)] * 2 + [pieces] * 8
        scratch += [vm((nd, 2 * depth, ch // 2), BF16)] * 4
        scratch += [dma((2, nl // 2))] * 4 + [dma((2, nd))] * 2
        grad_shape = (2 * depth, ch // 2)
    else:
        grad_shape = (taps_rows, ch)
    any_spec = pl.BlockSpec(memory_space=pl.ANY)
    vmem_spec = pl.BlockSpec(memory_space=pltpu.VMEM)
    place = vm if scatter else jax.ShapeDtypeStruct
    ig, g1, g2 = pl.pallas_call(
        functools.partial(kernel, nl, nd, scatter, norm),
        out_shape=(
            place(inputs.shape, BF16),
            place(grad_shape, F32),
            place(grad_shape, F32),
        ),
        in_specs=[any_spec] * 5,
        out_specs=(vmem_spec, vmem_spec, vmem_spec),
        scratch_shapes=scratch,
        compiler_params=pltpu.CompilerParams(
            collective_id=0, has_side_effects=True, vmem_limit_bytes=62 * 1024 * 1024
        ),
        name="conv_backward",
    )(inputs, pre_act, cotangent, first_weight, second_weight)
    if scatter:
        ig, g1, g2 = emit(ig, g1, g2)
    g1, g2 = g1.reshape(-1), g2.reshape(-1)
    if not scatter:
        g1, g2 = (lax.psum_scatter(g, "lon", scatter_dimension=0, tiled=True) for g in (g1, g2))
        g1, g2 = (lax.psum_scatter(g, "dp", scatter_dimension=0, tiled=True) for g in (g1, g2))
    return ig, g1, g2


def solution(mesh):
    in_specs = (
        P("dp", None, "lon", None),
        P("dp", None, "lon", None),
        P("dp", None, "lon", None),
        P(),
        P(),
    )
    out_specs = (P("dp", None, "lon", None), P(("lon", "dp")), P(("lon", "dp")))
    step = functools.partial(local, mesh.shape["lon"], mesh.shape["dp"])
    return jax.shard_map(step, mesh=mesh, in_specs=in_specs, out_specs=out_specs, check_vma=False)
```

```python
import functools

import jax
import jax.numpy as jnp
from jax import lax
from jax.experimental import pallas as pl
from jax.experimental.pallas import tpu as pltpu
from jax.sharding import PartitionSpec as P

FIRST_SPREAD = 12
SECOND_SPREAD = 18
MESH = pl.DeviceIdType.MESH
F32 = jnp.float32
BF16 = jnp.bfloat16
LANE_SLOT = (0, 2, 1)


def row_span(rows, dilation, r):
    if r == 0:
        return 0, rows - dilation, dilation
    if r == 1:
        return 0, rows, 0
    return dilation, rows, 0


def row_blocks(rows, dilation):
    cuts = sorted({0, dilation, rows - dilation, rows})
    blocks = []
    for lo, hi in zip(cuts, cuts[1:]):
        taps = []
        for r in range(3):
            start, stop, first = row_span(rows, dilation, r)
            if start <= lo and hi <= stop:
                taps.append((r, first + lo - start))
        blocks.append((lo, hi, taps))
    return blocks


def dot_nt(a, b):
    return lax.dot_general(a, b, (((1,), (1,)), ((), ())), preferred_element_type=F32)


def dot_tn(a, b):
    return lax.dot_general(a, b, (((0,), (0,)), ((), ())), preferred_element_type=F32)


def flat(v):
    return v.reshape(-1, v.shape[-1])


def kernel(nl, nd, scatter, norm, *refs):
    refs = list(refs)

    def take(count):
        taken = refs[:count]
        del refs[:count]
        return taken

    inp, pre, cot, w1, w2 = take(5)
    ig_out, g1_out, g2_out = take(3)
    pre_v, inp_v, w1_v, w2_v, side2, side1, acc = take(7)
    cot_e, pre_e, inp_e, acc_e = take(4)
    in_sem, w1_sem, w2_sem = take(3)
    sa, ra, sb, rb, sc, rc, hs_sem, hr_sem = take(8)
    if scatter:
        dw1, dw2 = take(2)
        sums = [take(10) for _ in range(2)]
        p_ssem, p_rsem, a_ssem, a_rsem, b_ssem, b_rsem, c_ssem, c_rsem, d_ssem, d_rsem = take(10)
    else:
        dw1, dw2 = g1_out, g2_out

    rows, cols, ch = pre_v.shape
    first_d, second_d = FIRST_SPREAD, SECOND_SPREAD
    rest = second_d - first_d
    me_l, me_d = lax.axis_index("lon"), lax.axis_index("dp")
    left, right = lax.rem(me_l + nl - 1, nl), lax.rem(me_l + 1, nl)
    half = nl // 2
    core = lax.rem(me_l, 2)
    my_chip = me_l // 2
    cot_v = side2.at[:, :, pl.ds(2 * ch, ch)]
    lg_v = side1.at[:, :, pl.ds(2 * ch, ch)]
    section = pl.when(me_l >= 0)

    def plane_device(t):
        return (2 * lax.rem(my_chip + t, half) + core, me_d)

    def depth_device(u):
        return (me_l, lax.rem(me_d + u, nd))

    load_cot = pltpu.make_async_copy(cot.at[0], cot_v, in_sem.at[0])
    load_pre = pltpu.make_async_copy(pre.at[0], pre_v, in_sem.at[1])
    load_inp = pltpu.make_async_copy(inp.at[0], inp_v, in_sem.at[2])

    def weight_loads(w, w_v, sem):
        return [
            pltpu.make_async_copy(
                w.at[pl.ds(k * ch, ch)],
                w_v.at[k // 3, :, pl.ds(LANE_SLOT.index(k % 3) * ch, ch)],
                sem.at[k],
            )
            for k in range(9)
        ]

    load_w2 = weight_loads(w2, w2_v, w2_sem)
    load_w1 = weight_loads(w1, w1_v, w1_sem)
    load_cot.start()

    barrier = pltpu.get_barrier_semaphore()
    for other in (left, right):
        pl.semaphore_signal(barrier, inc=1, device_id=(other, me_d), device_id_type=MESH)
    greeted = 2
    if scatter:
        for t in range(1, half):
            pl.semaphore_signal(barrier, inc=1, device_id=plane_device(t), device_id_type=MESH)
        for u in range(1, nd):
            pl.semaphore_signal(barrier, inc=1, device_id=depth_device(u), device_id_type=MESH)
        greeted += half - 1 + nd - 1
    for c in load_w2:
        c.start()
    load_pre.start()
    load_inp.start()
    for c in load_w1:
        c.start()

    def halo_copies(send, recv, base):
        return [
            pltpu.make_async_remote_copy(
                src_ref=send.at[i], dst_ref=recv.at[i], send_sem=hs_sem.at[base + i],
                recv_sem=hr_sem.at[base + i], device_id=(other, me_d), device_id_type=MESH,
            )
            for i, other in enumerate((left, right))
        ]

    def pack(dst, src, start, width):
        for p in range(rows):
            dst[p * width : (p + 1) * width, :] = src[p, start : start + width, :]

    def side_inner(src, side, d):
        side[:, 0 : cols - d, 0:ch] = src[:, d:cols, :]
        side[:, d:cols, ch : 2 * ch] = src[:, 0 : cols - d, :]

    def side_fill(side, piece, lo_at, hi_at, width):
        side[:, lo_at : lo_at + width, 0:ch] = piece[0].reshape(rows, width, ch)
        side[:, hi_at : hi_at + width, ch : 2 * ch] = piece[1].reshape(rows, width, ch)

    def input_terms(src, at, lanes, w_v, wl, d, fresh):
        for r in (1, 0, 2):
            lo, hi, first = row_span(rows, d, r)
            term = dot_nt(
                flat(src[first : first + hi - lo, :, at : at + lanes]),
                w_v[r, :, wl : wl + lanes],
            )
            if fresh and r == 1:
                acc[...] = term
            else:
                acc[lo * cols : hi * cols, :] += term

    def scaled(value):
        return value if scatter else value * norm

    def weight_terms(x, src, at, lanes, dw, taps, d):
        for r in range(3):
            lo, hi, first = row_span(rows, d, r)
            term = dot_tn(flat(x[lo:hi]), flat(src[first : first + hi - lo, :, at : at + lanes]))
            for i, c in enumerate(taps):
                k = 3 * r + c
                dw[k * ch : (k + 1) * ch, :] = scaled(term[:, i * ch : (i + 1) * ch])

    def edge_terms(out, lo, hi, taps, width, parts, w_v):
        total = None
        for strip, slot in parts:
            for r, first in taps:
                term = dot_nt(
                    strip[first * width : (first + hi - lo) * width, :],
                    w_v[r, :, slot * ch : (slot + 1) * ch],
                )
                total = term if total is None else total + term
        return total

    if scatter:
        depth = dw1.shape[0] // (nl * nd)
        cut = depth * 2 // 24 * 8
        plane_order = (*range(1, half), 0)

        def chunk(dw, s, parity, start, stop):
            l, d = 2 * (s // nd) + parity, lax.rem(s, nd)
            at = pl.multiple_of((l * nd + d) * depth, 8)
            return dw[pl.ds(at + start, stop - start), :]

        def remote(src, dst, send, recv, device):
            return pltpu.make_async_remote_copy(
                src_ref=src, dst_ref=dst, send_sem=send, recv_sem=recv,
                device_id=device, device_id_type=MESH,
            )

        def pair_copy(g, t):
            ps, pr = sums[g][:2]
            part = pl.ds(lax.rem(my_chip + t, half) * nd, nd)
            sibling = (me_l + 1 - 2 * core, me_d)
            return remote(ps.at[part], pr.at[part], p_ssem.at[g, t], p_rsem.at[g, t], sibling)

        def plane_copy(g, t):
            s, r = sums[g][2:4]
            part = pl.ds(lax.rem(my_chip + t, half) * nd, nd)
            return remote(
                s.at[part], r.at[pl.ds(t * nd, nd)],
                a_ssem.at[g, t], a_rsem.at[g, t], plane_device(t),
            )

        def plane_depth_copy(g, u):
            s, r = sums[g][4:6]
            return remote(s.at[u], r.at[u], b_ssem.at[g, u], b_rsem.at[g, u], depth_device(u))

        def depth_copy(g, u):
            s, r = sums[g][6:8]
            return remote(s.at[u], r.at[u], c_ssem.at[g, u], c_rsem.at[g, u], depth_device(u))

        def depth_plane_copy(g, t):
            s, r = sums[g][8:10]
            return remote(s.at[t], r.at[t], d_ssem.at[g, t], d_rsem.at[g, t], plane_device(t))

        def pair_send(g, dw):
            ps = sums[g][0]
            for t in plane_order:
                for d in range(nd):
                    s = lax.rem(my_chip + t, half) * nd + d
                    ps[s] = chunk(dw, s, 1 - core, 0, depth).astype(BF16)
                pair_copy(g, t).start()

        def chip_sum(g, dw, s, start, stop):
            pr = sums[g][1]
            return chunk(dw, s, core, start, stop) + pr[s, start:stop, :].astype(F32)

        def first_stage(g, dw):
            plane_s, depth_s = sums[g][2], sums[g][6]
            for t in plane_order:
                pair_copy(g, t).wait()
                if t == 0:
                    continue
                for d in range(nd):
                    s = lax.rem(my_chip + t, half) * nd + d
                    plane_s[s] = chip_sum(g, dw, s, 0, cut).astype(BF16)
                plane_copy(g, t).start()
            for u in range(1, nd):
                for c in range(half):
                    s = c * nd + lax.rem(me_d + u, nd)
                    depth_s[u, c] = chip_sum(g, dw, s, cut, depth).astype(BF16)
                depth_copy(g, u).start()

        def plane_sum(g, dw, d):
            total = chip_sum(g, dw, my_chip * nd + d, 0, cut)
            for t in range(1, half):
                total += sums[g][3][t * nd + d].astype(F32)
            return total

        def depth_sum(g, dw, c):
            total = chip_sum(g, dw, c * nd + me_d, cut, depth)
            for u in range(1, nd):
                total += sums[g][7][u, c].astype(F32)
            return total

        def second_stage(g, dw):
            for t in range(1, half):
                plane_copy(g, t).wait()
            for u in range(1, nd):
                sums[g][4][u] = plane_sum(g, dw, lax.rem(me_d + u, nd)).astype(BF16)
                plane_depth_copy(g, u).start()
            for u in range(1, nd):
                depth_copy(g, u).wait()
            for t in range(1, half):
                c = lax.rem(my_chip + t, half)
                sums[g][8][t] = depth_sum(g, dw, c).astype(BF16)
                depth_plane_copy(g, t).start()

        def last_stage(g, dw, out):
            total = plane_sum(g, dw, me_d)
            for u in range(1, nd):
                plane_depth_copy(g, u).wait()
                total += sums[g][5][u].astype(F32)
            for i in range(2):
                out[pl.ds(i, cut, stride=2), :] = total[:, i * ch // 2 : (i + 1) * ch // 2] * norm
            total = depth_sum(g, dw, my_chip)
            for t in range(1, half):
                depth_plane_copy(g, t).wait()
                total += sums[g][9][t].astype(F32)
            for i in range(2):
                out[pl.ds(2 * cut + i, depth - cut, stride=2), :] = (
                    total[:, i * ch // 2 : (i + 1) * ch // 2] * norm
                )

    load_cot.wait()
    pack(sa.at[0], cot_v, rest, first_d)
    pack(sa.at[1], cot_v, cols - second_d, first_d)
    pack(sb.at[0], cot_v, 0, rest)
    pack(sb.at[1], cot_v, cols - rest, rest)
    pl.semaphore_wait(barrier, greeted)
    halo_a = halo_copies(sa, ra, 0)
    halo_b = halo_copies(sb, rb, 2)
    for c in halo_a + halo_b:
        c.start()

    @section
    def _():
        side_inner(cot_v, side2, second_d)
        pack(cot_e.at[0], cot_v, 0, first_d)
        pack(cot_e.at[1], cot_v, cols - first_d, first_d)
        pack(cot_e.at[2], cot_v, second_d, first_d)
        pack(cot_e.at[3], cot_v, cols - first_d - second_d, first_d)

    for c in load_w2:
        c.wait()
    strips = ((0, 2, 2, 0, 1), (1, 2, 3, 1, 0))

    @section
    def _():
        for e, own, other, slot, _ in strips:
            for lo, hi, taps in row_blocks(rows, second_d):
                acc_e[e, lo * first_d : hi * first_d, :] = edge_terms(
                    None, lo, hi, taps, first_d,
                    ((cot_e.at[e], own), (cot_e.at[other], slot)), w2_v,
                )

    @section
    def _():
        input_terms(side2, 2 * ch, ch, w2_v, 2 * ch, second_d, True)

    load_pre.wait()

    @section
    def _():
        pre_v[...] = jnp.maximum(pre_v[...], jnp.zeros((), BF16))
        pack(pre_e.at[0], pre_v, 0, first_d)
        pack(pre_e.at[1], pre_v, cols - first_d, first_d)
        weight_terms(pre_v, side2, 2 * ch, ch, dw2, (1,), second_d)

    for c in halo_a:
        c.wait()

    @section
    def _():
        for e, _, _, _, slot in strips:
            for lo, hi, taps in row_blocks(rows, second_d):
                part = slice(lo * first_d, hi * first_d)
                grad = acc_e[e, part, :] + edge_terms(
                    None, lo, hi, taps, first_d, ((ra.at[1 - e], slot),), w2_v
                )
                sc[e, part, :] = jnp.where(pre_e[e, part, :] > 0, grad, F32(0.0)).astype(BF16)

    halo_c = halo_copies(sc, rc, 4)
    for c in halo_c:
        c.start()

    @section
    def _():
        side_fill(side2, ra, cols - first_d, 0, first_d)

    for c in halo_b:
        c.wait()

    @section
    def _():
        side_fill(side2, rb, cols - second_d, first_d, rest)

    @section
    def _():
        input_terms(side2, 0, 2 * ch, w2_v, 0, second_d, False)

    @section
    def _():
        grad = jnp.where(flat(pre_v[...]) > 0, acc[...], F32(0.0)).astype(BF16)
        lg_v[...] = grad.reshape(rows, cols, ch)

    @section
    def _():
        weight_terms(pre_v, side2, 0, 2 * ch, dw2, (0, 2), second_d)

    if scatter:
        pair_send(1, dw2)
    load_inp.wait()

    @section
    def _():
        zero = jnp.zeros((rows, first_d, ch), BF16)
        side1[:, cols - first_d : cols, 0:ch] = zero
        side1[:, 0:first_d, ch : 2 * ch] = zero
        side_inner(lg_v, side1, first_d)
        pack(inp_e.at[0], inp_v, 0, first_d)
        pack(inp_e.at[1], inp_v, cols - first_d, first_d)

    @section
    def _():
        weight_terms(inp_v, side1, 0, 3 * ch, dw1, (0, 2, 1), first_d)

    if scatter:
        first_stage(1, dw2)
    for c in halo_c:
        c.wait()

    @section
    def _():
        for r in range(3):
            lo, hi, first = row_span(rows, first_d, r)
            for e, c in ((1, 0), (0, 2)):
                k = 3 * r + c
                term = dot_tn(
                    inp_e[e, lo * first_d : hi * first_d, :],
                    rc[1 - e, first * first_d : (first + hi - lo) * first_d, :],
                )
                dw1[k * ch : (k + 1) * ch, :] += scaled(term)

    if scatter:
        pair_send(0, dw1)

    @section
    def _():
        side_fill(side1, rc, cols - first_d, 0, first_d)

    for c in load_w1:
        c.wait()
    if scatter:
        first_stage(0, dw1)

    @section
    def _():
        input_terms(side1, 0, 3 * ch, w1_v, 0, first_d, True)
        ig_out[0] = acc[...].astype(BF16).reshape(rows, cols, ch)

    if scatter:
        second_stage(1, dw2)
        second_stage(0, dw1)
        last_stage(1, dw2, g2_out)
        last_stage(0, dw1, g1_out)


def emit_kernel(*refs):
    count = len(refs) // 2
    copies = [
        pltpu.make_async_copy(refs[i], refs[count + i], refs[-1].at[i]) for i in range(count)
    ]
    for c in copies:
        c.start()
    for c in copies:
        c.wait()


def emit(*values):
    any_spec = pl.BlockSpec(memory_space=pl.ANY)
    vmem_spec = pl.BlockSpec(memory_space=pltpu.VMEM)
    return pl.pallas_call(
        emit_kernel,
        out_shape=[jax.ShapeDtypeStruct(v.shape, v.dtype) for v in values],
        in_specs=[vmem_spec] * len(values),
        out_specs=[any_spec] * len(values),
        scratch_shapes=[pltpu.SemaphoreType.DMA((len(values),))],
        name="emit",
    )(*(pltpu.with_memory_space_constraint(v, pltpu.VMEM) for v in values))


def local(nl, nd, inputs, pre_act, cotangent, first_weight, second_weight):
    _, rows, cols, ch = inputs.shape
    taps_rows = first_weight.shape[0]
    norm = float(rows * cols * nl * inputs.shape[0] * nd) ** -0.5
    devices = nl * nd
    depth = taps_rows // devices
    scatter = nl % 2 == 0 and taps_rows % devices == 0 and depth % 8 == 0 and depth >= 16
    slots = devices // 2
    vm = pltpu.VMEM
    dma = pltpu.SemaphoreType.DMA
    field = vm((rows, cols, ch), BF16)
    weights = vm((3, ch, 3 * ch), BF16)
    side = vm((rows, cols, 3 * ch), BF16)
    rest = SECOND_SPREAD - FIRST_SPREAD

    def strip(count, width, dtype=BF16):
        return vm((count, rows * width, ch), dtype)

    scratch = [field] * 2 + [weights] * 2 + [side] * 2 + [vm((rows * cols, ch), F32)]
    scratch += [strip(4, FIRST_SPREAD), strip(2, FIRST_SPREAD), strip(2, FIRST_SPREAD)]
    scratch += [strip(2, FIRST_SPREAD, F32)]
    scratch += [dma((3,)), dma((9,)), dma((9,))]
    scratch += [strip(2, FIRST_SPREAD)] * 2 + [strip(2, rest)] * 2 + [strip(2, FIRST_SPREAD)] * 2
    scratch += [dma((6,)), dma((6,))]
    if scatter:
        half = nl // 2
        cut = depth * 2 // 24 * 8
        scratch += [vm((taps_rows, ch), F32)] * 2
        for _ in range(2):
            scratch += [vm((slots, depth, ch), BF16)] * 2
            scratch += [vm((slots, cut, ch), BF16)] * 2
            scratch += [vm((nd, cut, ch), BF16)] * 2
            scratch += [vm((nd, half, depth - cut, ch), BF16)] * 2
            scratch += [vm((half, depth - cut, ch), BF16)] * 2
        for count in (half, half, nd, nd, half):
            scratch += [dma((2, count))] * 2
        grad_shape = (2 * depth, ch // 2)
    else:
        grad_shape = (taps_rows, ch)
    any_spec = pl.BlockSpec(memory_space=pl.ANY)
    vmem_spec = pl.BlockSpec(memory_space=pltpu.VMEM)
    place = vm if scatter else jax.ShapeDtypeStruct
    ig, g1, g2 = pl.pallas_call(
        functools.partial(kernel, nl, nd, scatter, norm),
        out_shape=(
            place(inputs.shape, BF16),
            place(grad_shape, F32),
            place(grad_shape, F32),
        ),
        in_specs=[any_spec] * 5,
        out_specs=(vmem_spec, vmem_spec, vmem_spec),
        scratch_shapes=scratch,
        compiler_params=pltpu.CompilerParams(
            collective_id=0, has_side_effects=True, vmem_limit_bytes=62 * 1024 * 1024
        ),
        name="conv_backward",
    )(inputs, pre_act, cotangent, first_weight, second_weight)
    if scatter:
        ig, g1, g2 = emit(ig, g1, g2)
    g1, g2 = g1.reshape(-1), g2.reshape(-1)
    if not scatter:
        g1, g2 = (lax.psum_scatter(g, "lon", scatter_dimension=0, tiled=True) for g in (g1, g2))
        g1, g2 = (lax.psum_scatter(g, "dp", scatter_dimension=0, tiled=True) for g in (g1, g2))
    return ig, g1, g2


def solution(mesh):
    in_specs = (
        P("dp", None, "lon", None),
        P("dp", None, "lon", None),
        P("dp", None, "lon", None),
        P(),
        P(),
    )
    out_specs = (P("dp", None, "lon", None), P(("lon", "dp")), P(("lon", "dp")))
    step = functools.partial(local, mesh.shape["lon"], mesh.shape["dp"])
    return jax.shard_map(step, mesh=mesh, in_specs=in_specs, out_specs=out_specs, check_vma=False)
```

```python
import functools
import typing

import jax
import jax.numpy as jnp
from jax import lax
from jax.experimental import pallas as pl
from jax.experimental.pallas import tpu as pltpu
from jax.sharding import PartitionSpec as P

FIRST_SPREAD = 12
SECOND_SPREAD = 18
MESH = pl.DeviceIdType.MESH
F32 = jnp.float32
BF16 = jnp.bfloat16
LANE_SLOT = (0, 2, 1)


def row_span(rows, dilation, r):
    if r == 0:
        return 0, rows - dilation, dilation
    if r == 1:
        return 0, rows, 0
    return dilation, rows, 0


class Bank(typing.NamedTuple):
    ep_s: typing.Any
    ep_r: typing.Any
    ez_s: typing.Any
    ez_r: typing.Any
    ex_s: typing.Any
    ex_r: typing.Any
    lp_s: typing.Any
    lp_r: typing.Any
    pa_s: typing.Any
    pa_r: typing.Any
    pb_s: typing.Any
    pb_r: typing.Any
    za_s: typing.Any
    za_r: typing.Any
    zb_s: typing.Any
    zb_r: typing.Any
    ep_sem: typing.Any
    ez_sem: typing.Any
    ex_sem: typing.Any
    lps_sem: typing.Any
    lpr_sem: typing.Any
    pas_sem: typing.Any
    par_sem: typing.Any
    pbs_sem: typing.Any
    pbr_sem: typing.Any
    za_sem: typing.Any
    zb_sem: typing.Any


def first_rows(depth):
    return depth * 8 // 72 * 8, depth * 7 // 72 * 8


def bank_scratch(nl, nd, depth, ch, cut):
    half = nl // 2
    dma = pltpu.SemaphoreType.DMA

    def buf(*shape):
        return pltpu.VMEM((*shape, ch), BF16)

    return [
        *[buf(nd, depth)] * 4, buf(depth), buf(half, depth),
        *[buf(half - 1, nd, depth)] * 2,
        buf(nd, half - 1, cut), buf(nd, half, cut), *[buf(nd, cut)] * 2,
        *[buf(nd, half - 1, depth - cut)] * 2, buf(half - 1, depth - cut), buf(half, depth - cut),
        dma((2,)), dma((2,)), dma((2,)), dma, dma((half - 1,)),
        dma((nd,)), dma((nd,)), dma((nd,)), dma, dma((2,)), dma((2,)),
    ]


def early_owners(nl, nd, depth, ch):
    table = []
    for parity in range(2):
        row = []
        for d in range(nd):
            chips = []
            for chip in range(nl // 2):
                start = ((2 * chip + parity) * nd + d) * depth
                taps = {start // ch % 3, (start + depth - 1) // ch % 3}
                if taps == {1} and depth <= ch:
                    chips.append(chip)
            if len(chips) != 1:
                return None
            row.append(chips[0])
        table.append(row)
    return table


def row_blocks(rows, dilation):
    cuts = sorted({0, dilation, rows - dilation, rows})
    blocks = []
    for lo, hi in zip(cuts, cuts[1:]):
        taps = []
        for r in range(3):
            start, stop, first = row_span(rows, dilation, r)
            if start <= lo and hi <= stop:
                taps.append((r, first + lo - start))
        blocks.append((lo, hi, taps))
    return blocks


def dot_nt(a, b):
    return lax.dot_general(a, b, (((1,), (1,)), ((), ())), preferred_element_type=F32)


def dot_tn(a, b):
    return lax.dot_general(a, b, (((0,), (0,)), ((), ())), preferred_element_type=F32)


def flat(v):
    return v.reshape(-1, v.shape[-1])


def kernel(nl, nd, owners, norm, *refs):
    refs = list(refs)
    scatter = owners is not None

    def take(count):
        taken = refs[:count]
        del refs[:count]
        return taken

    inp, pre, cot, w1, w2 = take(5)
    ig_out, g1_out, g2_out = take(3)
    pre_v, inp_v, w1_v, w2_v, side2, side1, acc = take(7)
    cot_e, pre_e, inp_e, acc_e, cot_f, pre_f, acc_f, lg_f = take(8)
    in_sem, w1_sem, w2_sem = take(3)
    sa, ra, sb, rb, sc, rc, hs_sem, hr_sem = take(8)
    if scatter:
        dw1, dw2 = take(2)
        banks = [Bank(*take(len(Bank._fields))) for _ in range(2)]
        (greet,) = take(1)
    else:
        dw1, dw2 = g1_out, g2_out

    rows, cols, ch = pre_v.shape
    first_d, second_d = FIRST_SPREAD, SECOND_SPREAD
    rest = second_d - first_d
    me_l, me_d = lax.axis_index("lon"), lax.axis_index("dp")
    left, right = lax.rem(me_l + nl - 1, nl), lax.rem(me_l + 1, nl)
    half = nl // 2
    core = lax.rem(me_l, 2)
    my_chip = me_l // 2
    cot_v = side2.at[:, :, pl.ds(2 * ch, ch)]
    lg_v = side1.at[:, :, pl.ds(2 * ch, ch)]
    section = pl.when(me_l >= 0)

    def plane_device(t):
        return (2 * lax.rem(my_chip + t, half) + core, me_d)

    def depth_device(u):
        return (me_l, lax.rem(me_d + u, nd))

    load_cot = pltpu.make_async_copy(cot.at[0], cot_v, in_sem.at[0])
    load_pre = pltpu.make_async_copy(pre.at[0], pre_v, in_sem.at[1])
    load_inp = pltpu.make_async_copy(inp.at[0], inp_v, in_sem.at[2])

    def weight_loads(w, w_v, sem):
        return [
            pltpu.make_async_copy(
                w.at[pl.ds(k * ch, ch)],
                w_v.at[k // 3, :, pl.ds(LANE_SLOT.index(k % 3) * ch, ch)],
                sem,
            )
            for k in range(9)
        ]

    load_w2 = weight_loads(w2, w2_v, w2_sem)
    load_w1 = weight_loads(w1, w1_v, w1_sem)

    def landed(ref, sem):
        pltpu.make_async_copy(ref, ref, sem).wait()

    load_cot.start()

    barrier = pltpu.get_barrier_semaphore()
    for other in (left, right):
        pl.semaphore_signal(barrier, inc=1, device_id=(other, me_d), device_id_type=MESH)
    greeted = 2
    if scatter:
        for t in range(1, half):
            pl.semaphore_signal(barrier, inc=1, device_id=plane_device(t), device_id_type=MESH)
        for d in range(1, nd):
            @pl.when(me_d < d)
            def _(d=d):
                pl.semaphore_signal(barrier, inc=1, device_id=(me_l, d), device_id_type=MESH)
        greeted += half - 1 + me_d
    for c in load_w2:
        c.start()
    load_pre.start()
    load_inp.start()
    for c in load_w1:
        c.start()

    def halo_copies(send, recv, base):
        return [
            pltpu.make_async_remote_copy(
                src_ref=send.at[i], dst_ref=recv.at[i], send_sem=hs_sem.at[base],
                recv_sem=hr_sem.at[base], device_id=(other, me_d), device_id_type=MESH,
            )
            for i, other in enumerate((left, right))
        ]

    def pack(dst, src, start, width):
        for p in range(rows):
            dst[p * width : (p + 1) * width, :] = src[p, start : start + width, :]

    def side_inner(src, side, d):
        zero = jnp.zeros((rows, d, ch), BF16)
        side[:, cols - d : cols, 0:ch] = zero
        side[:, 0:d, ch : 2 * ch] = zero
        side[:, 0 : cols - d, 0:ch] = src[:, d:cols, :]
        side[:, d:cols, ch : 2 * ch] = src[:, 0 : cols - d, :]

    def side_fill(side, piece, lo_at, hi_at, width):
        side[:, lo_at : lo_at + width, 0:ch] = piece[0].reshape(rows, width, ch)
        side[:, hi_at : hi_at + width, ch : 2 * ch] = piece[1].reshape(rows, width, ch)

    def input_terms(src, at, lanes, w_v, wl, d, fresh):
        for r in (1, 0, 2):
            lo, hi, first = row_span(rows, d, r)
            term = dot_nt(
                flat(src[first : first + hi - lo, :, at : at + lanes]),
                w_v[r, :, wl : wl + lanes],
            )
            if fresh and r == 1:
                acc[...] = term
            else:
                acc[lo * cols : hi * cols, :] += term

    def scaled(value):
        return value if scatter else value * norm

    def weight_terms(x, src, at, lanes, dw, taps, d):
        for r in range(3):
            lo, hi, first = row_span(rows, d, r)
            term = dot_tn(flat(x[lo:hi]), flat(src[first : first + hi - lo, :, at : at + lanes]))
            for i, c in enumerate(taps):
                k = 3 * r + c
                dw[k * ch : (k + 1) * ch, :] = scaled(term[:, i * ch : (i + 1) * ch])

    def edge_terms(lo, hi, taps, width, parts, w_v):
        total = None
        for strip, slot in parts:
            for r, first in taps:
                term = dot_nt(
                    strip[first * width : (first + hi - lo) * width, :],
                    w_v[r, :, slot * ch : (slot + 1) * ch],
                )
                total = term if total is None else total + term
        return total

    if scatter:
        depth = dw1.shape[0] // (nl * nd)

        def owner(parity, d):
            total = 0
            for dd in range(nd):
                low, high = owners[0][dd], owners[1][dd]
                total = jnp.where(d == dd, low + parity * (high - low), total)
            return total

        def late(parity, d, i):
            return i + jnp.where(owner(parity, d) <= i, 1, 0)

        def chunk(dw, chip, d, parity, start, stop):
            at = pl.multiple_of(((2 * chip + parity) * nd + d) * depth, 8)
            return dw[pl.ds(at + start, stop - start), :]

        def remote(src, dst, send, recv, device):
            return pltpu.make_async_remote_copy(
                src_ref=src, dst_ref=dst, send_sem=send, recv_sem=recv,
                device_id=device, device_id_type=MESH,
            )

        def seen_from(chip):
            return lax.rem(my_chip - chip + half, half)

        sibling = (me_l + 1 - 2 * core, me_d)
        mine = owner(core, me_d)

        def early_pair(g, dw):
            b = banks[g]
            for d in range(nd):
                chip = owner(1 - core, d)
                b.ep_s[d] = chunk(dw, chip, d, 1 - core, 0, depth).astype(BF16)
            remote(b.ep_s, b.ep_r, b.ep_sem.at[0], b.ep_sem.at[1], sibling).start()

        def early_chip_sum(b, dw, d):
            return chunk(dw, owner(core, d), d, core, 0, depth) + b.ep_r[d].astype(F32)

        def early_depth(g, dw):
            b = banks[g]
            landed(b.ep_r, b.ep_sem.at[1])
            for u in range(1, nd):
                b.ez_s[u] = early_chip_sum(b, dw, lax.rem(me_d + u, nd)).astype(BF16)
                remote(
                    b.ez_s.at[u], b.ez_r.at[u], b.ez_sem.at[0], b.ez_sem.at[1], depth_device(u)
                ).start()

        def early_sum(b, dw):
            total = early_chip_sum(b, dw, me_d)
            for u in range(1, nd):
                total += b.ez_r[u].astype(F32)
            return total

        def early_plane(g, dw):
            b = banks[g]
            landed(b.ez_r.at[pl.ds(1, nd - 1)], b.ez_sem.at[1])

            @pl.when(my_chip != mine)
            def _():
                b.ex_s[...] = early_sum(b, dw).astype(BF16)
                remote(
                    b.ex_s, b.ex_r.at[seen_from(mine)], b.ex_sem.at[0], b.ex_sem.at[1],
                    (2 * mine + core, me_d),
                ).start()

        def late_pair(g, dw):
            b = banks[g]
            for i in range(half - 1):
                for d in range(nd):
                    chip = late(1 - core, d, i)
                    b.lp_s[i, d] = chunk(dw, chip, d, 1 - core, 0, depth).astype(BF16)
                remote(b.lp_s.at[i], b.lp_r.at[i], b.lps_sem, b.lpr_sem.at[i], sibling).start()

        def late_chip_sum(b, dw, chip, i, d, start, stop):
            return chunk(dw, chip, d, core, start, stop) + b.lp_r[i, d, start:stop, :].astype(F32)

        def late_first(g, dw):
            b = banks[g]
            for i in range(half - 1):
                landed(b.lp_r.at[i], b.lpr_sem.at[i])
                for d in range(nd):
                    chip = late(core, d, i)

                    @pl.when(chip != my_chip)
                    def _(i=i, d=d, chip=chip):
                        b.pa_s[d, i] = late_chip_sum(b, dw, chip, i, d, 0, b.pa_s.shape[2]).astype(BF16)
                        remote(
                            b.pa_s.at[d, i], b.pa_r.at[d, seen_from(chip)],
                            b.pas_sem.at[d], b.par_sem.at[d], (2 * chip + core, me_d),
                        ).start()
            for u in range(1, nd):
                d = lax.rem(me_d + u, nd)
                for i in range(half - 1):
                    chip = late(core, d, i)
                    b.za_s[u, i] = late_chip_sum(b, dw, chip, i, d, b.pa_s.shape[2], depth).astype(BF16)
                remote(
                    b.za_s.at[u], b.za_r.at[u], b.za_sem.at[0], b.za_sem.at[1], depth_device(u)
                ).start()

        def plane_sum(b, dw, d):
            i = my_chip - jnp.where(owner(core, d) < my_chip, 1, 0)
            total = late_chip_sum(b, dw, my_chip, i, d, 0, b.pa_s.shape[2])
            for t in range(1, half):
                total += b.pa_r[d, t].astype(F32)
            return total

        def depth_sum(b, dw, chip, i):
            total = late_chip_sum(b, dw, chip, i, me_d, b.pa_s.shape[2], depth)
            for u in range(1, nd):
                total += b.za_r[u, i].astype(F32)
            return total

        def late_second_plane(g, dw):
            b = banks[g]
            for u in (*range(1, nd), 0):
                d = lax.rem(me_d + u, nd)

                @pl.when(owner(core, d) != my_chip)
                def _(u=u, d=d):
                    landed(b.pa_r.at[d, pl.ds(1, half - 1)], b.par_sem.at[d])
                    if u:
                        b.pb_s[u] = plane_sum(b, dw, d).astype(BF16)
                        remote(
                            b.pb_s.at[u], b.pb_r.at[u], b.pbs_sem.at[u], b.pbr_sem,
                            depth_device(u),
                        ).start()

        def late_second_depth(g, dw):
            b = banks[g]
            landed(b.za_r.at[pl.ds(1, nd - 1)], b.za_sem.at[1])
            for i in range(half - 1):
                chip = late(core, me_d, i)

                @pl.when(chip != my_chip)
                def _(i=i, chip=chip):
                    b.zb_s[i] = depth_sum(b, dw, chip, i).astype(BF16)
                    remote(
                        b.zb_s.at[i], b.zb_r.at[seen_from(chip)],
                        b.zb_sem.at[0], b.zb_sem.at[1], (2 * chip + core, me_d),
                    ).start()

        def put(out, total, start, count):
            for i in range(2):
                out[pl.ds(2 * start + i, count, stride=2), :] = (
                    total[:, i * ch // 2 : (i + 1) * ch // 2] * norm
                )

        def last_stage(g, dw, out):
            b = banks[g]

            @pl.when(my_chip == mine)
            def _():
                total = early_sum(b, dw)
                landed(b.ex_r.at[pl.ds(1, half - 1)], b.ex_sem.at[1])
                for t in range(1, half):
                    total += b.ex_r[t].astype(F32)
                put(out, total, 0, depth)
                landed(b.zb_s, b.zb_sem.at[0])

            @pl.when(my_chip != mine)
            def _():
                landed(b.pb_r.at[pl.ds(1, nd - 1)], b.pbr_sem)
                total = plane_sum(b, dw, me_d)
                for u in range(1, nd):
                    total += b.pb_r[u].astype(F32)
                put(out, total, 0, b.pa_s.shape[2])
                landed(b.zb_r.at[pl.ds(1, half - 1)], b.zb_sem.at[1])
                total = depth_sum(b, dw, my_chip, my_chip - jnp.where(mine < my_chip, 1, 0))
                for t in range(1, half):
                    total += b.zb_r[t].astype(F32)
                put(out, total, b.pa_s.shape[2], depth - b.pa_s.shape[2])
                landed(b.zb_s.at[pl.ds(0, half - 2)], b.zb_sem.at[0])
                landed(b.ex_s, b.ex_sem.at[0])

            landed(b.ep_s, b.ep_sem.at[0])
            landed(b.ez_s.at[pl.ds(1, nd - 1)], b.ez_sem.at[0])
            landed(b.lp_s, b.lps_sem)
            landed(b.za_s.at[pl.ds(1, nd - 1)], b.za_sem.at[0])
            for u in range(nd):
                d = lax.rem(me_d + u, nd)

                @pl.when(owner(core, d) == my_chip)
                def _(d=d):
                    landed(b.pa_s.at[d], b.pas_sem.at[d])

                @pl.when(owner(core, d) != my_chip)
                def _(u=u, d=d):
                    landed(b.pa_s.at[d, pl.ds(0, half - 2)], b.pas_sem.at[d])
                    if u:
                        landed(b.pb_s.at[u], b.pbs_sem.at[u])

    load_cot.wait()
    pack(sa.at[0], cot_v, rest, first_d)
    pack(sa.at[1], cot_v, cols - second_d, first_d)
    pack(sb.at[0], cot_v, 0, rest)
    pack(sb.at[1], cot_v, cols - rest, rest)
    pl.semaphore_wait(barrier, greeted)
    if scatter:
        for d in range(nd - 1):
            @pl.when(me_d > d)
            def _(d=d):
                pl.semaphore_signal(greet, inc=1, device_id=(me_l, d), device_id_type=MESH)
    halo_a = halo_copies(sa, ra, 0)
    halo_b = halo_copies(sb, rb, 1)
    for c in halo_a + halo_b:
        c.start()

    outer = (cot_e, acc_e, first_d, (0, cols - first_d), (second_d, cols - first_d - second_d))
    inner = (
        cot_f, acc_f, rest, (first_d, cols - second_d),
        (first_d + second_d, cols - 2 * second_d),
    )

    def strip_packs(group):
        strips, _, width, own, other = group
        for e in range(2):
            pack(strips.at[e], cot_v, own[e], width)
            pack(strips.at[2 + e], cot_v, other[e], width)

    def strip_start(group):
        strips, sums_e, width, _, _ = group
        for e in range(2):
            for lo, hi, taps in row_blocks(rows, second_d):
                sums_e[e, lo * width : hi * width, :] = edge_terms(
                    lo, hi, taps, width, ((strips.at[e], 2), (strips.at[2 + e], e)), w2_v
                )

    def strip_finish(group, halo, pre_s, out):
        _, sums_e, width, _, _ = group
        for e in range(2):
            for lo, hi, taps in row_blocks(rows, second_d):
                part = slice(lo * width, hi * width)
                grad = sums_e[e, part, :] + edge_terms(
                    lo, hi, taps, width, ((halo.at[1 - e], 1 - e),), w2_v
                )
                out[e, part, :] = jnp.where(pre_s[e, part, :] > 0, grad, F32(0.0)).astype(BF16)

    def strip_place(group, value):
        _, _, width, own, _ = group
        for e in range(2):
            side1[:, own[e] : own[e] + width, 2 * ch : 3 * ch] = value[e].reshape(rows, width, ch)

    def edge_update(dw, d, groups):
        for r in range(3):
            lo, hi, first = row_span(rows, d, r)
            for e, c in ((1, 0), (0, 2)):
                total = None
                for own, halo, width in groups:
                    term = dot_tn(
                        own[e, lo * width : hi * width, :],
                        halo[1 - e, first * width : (first + hi - lo) * width, :],
                    )
                    total = term if total is None else total + term
                k = 3 * r + c
                dw[k * ch : (k + 1) * ch, :] += scaled(total)

    @section
    def _():
        side_inner(cot_v, side2, second_d)
        strip_packs(outer)
        strip_packs(inner)

    landed(w2_v, w2_sem)

    @section
    def _():
        strip_start(outer)

    load_pre.wait()

    @section
    def _():
        pre_v[...] = jnp.maximum(pre_v[...], jnp.zeros((), BF16))
        for e in range(2):
            pack(pre_e.at[e], pre_v, outer[3][e], first_d)
            pack(pre_f.at[e], pre_v, inner[3][e], rest)

    @section
    def _():
        input_terms(side2, 0, 3 * ch, w2_v, 0, second_d, True)

    @section
    def _():
        grad = jnp.where(flat(pre_v[...]) > 0, acc[...], F32(0.0)).astype(BF16)
        lg_v[...] = grad.reshape(rows, cols, ch)

    @section
    def _():
        weight_terms(pre_v, side2, 0, 3 * ch, dw2, (0, 2, 1), second_d)

    if scatter:
        early_pair(1, dw2)

    @section
    def _():
        strip_start(inner)

    landed(ra, hr_sem.at[0])

    @section
    def _():
        strip_finish(outer, ra, pre_e, sc)

    halo_c = halo_copies(sc, rc, 2)
    for c in halo_c:
        c.start()

    @section
    def _():
        strip_place(outer, sc)

    if scatter:
        @pl.when(me_d < nd - 1)
        def _():
            pl.semaphore_wait(greet, nd - 1 - me_d)

        early_depth(1, dw2)
    landed(rb, hr_sem.at[1])

    @section
    def _():
        strip_finish(inner, rb, pre_f, lg_f)
        strip_place(inner, lg_f)

    @section
    def _():
        edge_update(dw2, second_d, ((pre_e, ra, first_d), (pre_f, rb, rest)))

    if scatter:
        late_pair(1, dw2)
    load_inp.wait()

    @section
    def _():
        side_inner(lg_v, side1, first_d)
        pack(inp_e.at[0], inp_v, 0, first_d)
        pack(inp_e.at[1], inp_v, cols - first_d, first_d)

    @section
    def _():
        weight_terms(inp_v, side1, 0, 3 * ch, dw1, (0, 2, 1), first_d)

    if scatter:
        early_pair(0, dw1)
    if scatter:
        late_first(1, dw2)
    if scatter:
        early_depth(0, dw1)
    landed(rc, hr_sem.at[2])

    @section
    def _():
        edge_update(dw1, first_d, ((inp_e, rc, first_d),))

    if scatter:
        late_pair(0, dw1)

    @section
    def _():
        side_fill(side1, rc, cols - first_d, 0, first_d)

    landed(w1_v, w1_sem)
    if scatter:
        late_first(0, dw1)
    if scatter:
        early_plane(1, dw2)

    @section
    def _():
        input_terms(side1, 0, 3 * ch, w1_v, 0, first_d, True)
        ig_out[0] = acc[...].astype(BF16).reshape(rows, cols, ch)

    if scatter:
        late_second_plane(1, dw2)
    if scatter:
        late_second_depth(1, dw2)
    if scatter:
        late_second_plane(0, dw1)
    if scatter:
        late_second_depth(0, dw1)
    if scatter:
        early_plane(0, dw1)
    if scatter:
        last_stage(1, dw2, g2_out)
    if scatter:
        last_stage(0, dw1, g1_out)
    for i, ref in enumerate((sa, sb, sc)):
        landed(ref, hs_sem.at[i])


def emit_kernel(*refs):
    count = len(refs) // 2
    copies = [
        pltpu.make_async_copy(refs[i], refs[count + i], refs[-1].at[i]) for i in range(count)
    ]
    for c in copies:
        c.start()
    for c in copies:
        c.wait()


def emit(*values):
    any_spec = pl.BlockSpec(memory_space=pl.ANY)
    vmem_spec = pl.BlockSpec(memory_space=pltpu.VMEM)
    return pl.pallas_call(
        emit_kernel,
        out_shape=[jax.ShapeDtypeStruct(v.shape, v.dtype) for v in values],
        in_specs=[vmem_spec] * len(values),
        out_specs=[any_spec] * len(values),
        scratch_shapes=[pltpu.SemaphoreType.DMA((len(values),))],
        name="emit",
    )(*(pltpu.with_memory_space_constraint(v, pltpu.VMEM) for v in values))


def local(nl, nd, inputs, pre_act, cotangent, first_weight, second_weight):
    _, rows, cols, ch = inputs.shape
    taps_rows = first_weight.shape[0]
    norm = float(rows * cols * nl * inputs.shape[0] * nd) ** -0.5
    devices = nl * nd
    depth = taps_rows // devices
    even = nl % 2 == 0 and nl >= 6 and nd >= 2
    even = even and taps_rows % devices == 0 and depth % 8 == 0 and depth >= 16
    owners = early_owners(nl, nd, depth, ch) if even else None
    scatter = owners is not None
    vm = pltpu.VMEM
    dma = pltpu.SemaphoreType.DMA
    field = vm((rows, cols, ch), BF16)
    weights = vm((3, ch, 3 * ch), BF16)
    side = vm((rows, cols, 3 * ch), BF16)
    rest = SECOND_SPREAD - FIRST_SPREAD

    def strip(count, width, dtype=BF16):
        return vm((count, rows * width, ch), dtype)

    scratch = [field] * 2 + [weights] * 2 + [side] * 2 + [vm((rows * cols, ch), F32)]
    scratch += [strip(4, FIRST_SPREAD), strip(2, FIRST_SPREAD), strip(2, FIRST_SPREAD)]
    scratch += [strip(2, FIRST_SPREAD, F32)]
    scratch += [strip(4, rest), strip(2, rest), strip(2, rest, F32), strip(2, rest)]
    scratch += [dma((3,)), dma, dma]
    scratch += [strip(2, FIRST_SPREAD)] * 2 + [strip(2, rest)] * 2 + [strip(2, FIRST_SPREAD)] * 2
    scratch += [dma((3,)), dma((3,))]
    if scatter:
        scratch += [vm((taps_rows, ch), F32)] * 2
        for cut in first_rows(depth):
            scratch += bank_scratch(nl, nd, depth, ch, cut)
        scratch += [pltpu.SemaphoreType.REGULAR]
        grad_shape = (2 * depth, ch // 2)
    else:
        grad_shape = (taps_rows, ch)
    any_spec = pl.BlockSpec(memory_space=pl.ANY)
    vmem_spec = pl.BlockSpec(memory_space=pltpu.VMEM)
    place = vm if scatter else jax.ShapeDtypeStruct
    ig, g1, g2 = pl.pallas_call(
        functools.partial(kernel, nl, nd, owners, norm),
        out_shape=(
            place(inputs.shape, BF16),
            place(grad_shape, F32),
            place(grad_shape, F32),
        ),
        in_specs=[any_spec] * 5,
        out_specs=(vmem_spec, vmem_spec, vmem_spec),
        scratch_shapes=scratch,
        compiler_params=pltpu.CompilerParams(
            collective_id=0, has_side_effects=True, vmem_limit_bytes=62 * 1024 * 1024
        ),
        name="conv_backward",
    )(inputs, pre_act, cotangent, first_weight, second_weight)
    if scatter:
        ig, g1, g2 = emit(ig, g1, g2)
    g1, g2 = g1.reshape(-1), g2.reshape(-1)
    if not scatter:
        g1, g2 = (lax.psum_scatter(g, "lon", scatter_dimension=0, tiled=True) for g in (g1, g2))
        g1, g2 = (lax.psum_scatter(g, "dp", scatter_dimension=0, tiled=True) for g in (g1, g2))
    return ig, g1, g2


def solution(mesh):
    in_specs = (
        P("dp", None, "lon", None),
        P("dp", None, "lon", None),
        P("dp", None, "lon", None),
        P(),
        P(),
    )
    out_specs = (P("dp", None, "lon", None), P(("lon", "dp")), P(("lon", "dp")))
    step = functools.partial(local, mesh.shape["lon"], mesh.shape["dp"])
    return jax.shard_map(step, mesh=mesh, in_specs=in_specs, out_specs=out_specs, check_vma=False)
```

```python
import functools
import typing

import jax
import jax.numpy as jnp
from jax import lax
from jax.experimental import pallas as pl
from jax.experimental.pallas import tpu as pltpu
from jax.sharding import PartitionSpec as P

FIRST_SPREAD = 12
SECOND_SPREAD = 18
MESH = pl.DeviceIdType.MESH
F32 = jnp.float32
BF16 = jnp.bfloat16
LANE_SLOT = (0, 2, 1)


def row_span(rows, dilation, r):
    if r == 0:
        return 0, rows - dilation, dilation
    if r == 1:
        return 0, rows, 0
    return dilation, rows, 0


class Bank(typing.NamedTuple):
    ep_s: typing.Any
    ep_r: typing.Any
    ez_s: typing.Any
    ez_r: typing.Any
    ex_s: typing.Any
    ex_r: typing.Any
    lp_s: typing.Any
    lp_r: typing.Any
    pa_s: typing.Any
    pa_r: typing.Any
    pb_s: typing.Any
    pb_r: typing.Any
    za_s: typing.Any
    za_r: typing.Any
    zb_s: typing.Any
    zb_r: typing.Any
    ep_sem: typing.Any
    ez_sem: typing.Any
    ex_sem: typing.Any
    lps_sem: typing.Any
    lpr_sem: typing.Any
    pas_sem: typing.Any
    par_sem: typing.Any
    pbs_sem: typing.Any
    pbr_sem: typing.Any
    za_sem: typing.Any
    zb_sem: typing.Any


def first_rows(depth):
    return depth * 8 // 72 * 8, depth * 7 // 72 * 8


def bank_scratch(nl, nd, depth, ch, cut):
    half = nl // 2
    dma = pltpu.SemaphoreType.DMA

    def buf(*shape):
        return pltpu.VMEM((*shape, ch), BF16)

    return [
        *[buf(nd, depth)] * 4, buf(depth), buf(half, depth),
        *[buf(half - 1, nd, depth)] * 2,
        buf(nd, half - 1, cut), buf(nd, half, cut), *[buf(nd, cut)] * 2,
        *[buf(nd, half - 1, depth - cut)] * 2, buf(half - 1, depth - cut), buf(half, depth - cut),
        dma((2,)), dma((2,)), dma((2,)), dma, dma((half - 1,)),
        dma((nd,)), dma((nd,)), dma((nd,)), dma, dma((2,)), dma((2,)),
    ]


def early_owners(nl, nd, depth, ch):
    table = []
    for parity in range(2):
        row = []
        for d in range(nd):
            chips = []
            for chip in range(nl // 2):
                start = ((2 * chip + parity) * nd + d) * depth
                taps = {start // ch % 3, (start + depth - 1) // ch % 3}
                if taps == {1} and depth <= ch:
                    chips.append(chip)
            if len(chips) != 1:
                return None
            row.append(chips[0])
        table.append(row)
    return table


def row_blocks(rows, dilation):
    cuts = sorted({0, dilation, rows - dilation, rows})
    blocks = []
    for lo, hi in zip(cuts, cuts[1:]):
        taps = []
        for r in range(3):
            start, stop, first = row_span(rows, dilation, r)
            if start <= lo and hi <= stop:
                taps.append((r, first + lo - start))
        blocks.append((lo, hi, taps))
    return blocks


def dot_nt(a, b):
    return lax.dot_general(a, b, (((1,), (1,)), ((), ())), preferred_element_type=F32)


def dot_tn(a, b):
    return lax.dot_general(a, b, (((0,), (0,)), ((), ())), preferred_element_type=F32)


def flat(v):
    return v.reshape(-1, v.shape[-1])


def kernel(nl, nd, owners, norm, *refs):
    refs = list(refs)
    scatter = owners is not None

    def take(count):
        taken = refs[:count]
        del refs[:count]
        return taken

    inp, pre, cot, w1, w2 = take(5)
    ig_out, g1_out, g2_out = take(3)
    pre_v, inp_v, w1_v, w2_v, side2, side1, acc = take(7)
    cot_e, pre_e, inp_e, acc_e, cot_f, pre_f, acc_f, lg_f = take(8)
    in_sem, w1_sem, w2_sem = take(3)
    sa, ra, sb, rb, sc, rc, hs_sem, hr_sem = take(8)
    if scatter:
        dw1, dw2 = take(2)
        banks = [Bank(*take(len(Bank._fields))) for _ in range(2)]
        (greet,) = take(1)
    else:
        dw1, dw2 = g1_out, g2_out

    rows, cols, ch = pre_v.shape
    first_d, second_d = FIRST_SPREAD, SECOND_SPREAD
    rest = second_d - first_d
    me_l, me_d = lax.axis_index("lon"), lax.axis_index("dp")
    left, right = lax.rem(me_l + nl - 1, nl), lax.rem(me_l + 1, nl)
    half = nl // 2
    core = lax.rem(me_l, 2)
    my_chip = me_l // 2
    cot_v = side2.at[:, :, pl.ds(2 * ch, ch)]
    lg_v = side1.at[:, :, pl.ds(2 * ch, ch)]
    section = pl.when(me_l >= 0)

    def plane_device(t):
        return (2 * lax.rem(my_chip + t, half) + core, me_d)

    def depth_device(u):
        return (me_l, lax.rem(me_d + u, nd))

    load_cot = pltpu.make_async_copy(cot.at[0], cot_v, in_sem.at[0])
    load_pre = pltpu.make_async_copy(pre.at[0], pre_v, in_sem.at[1])
    load_inp = pltpu.make_async_copy(inp.at[0], inp_v, in_sem.at[2])

    def weight_loads(w, w_v, sem):
        return [
            pltpu.make_async_copy(
                w.at[pl.ds(k * ch, ch)],
                w_v.at[k // 3, :, pl.ds(LANE_SLOT.index(k % 3) * ch, ch)],
                sem,
            )
            for k in range(9)
        ]

    load_w2 = weight_loads(w2, w2_v, w2_sem)
    load_w1 = weight_loads(w1, w1_v, w1_sem)

    def landed(ref, sem):
        pltpu.make_async_copy(ref, ref, sem).wait()

    load_cot.start()

    barrier = pltpu.get_barrier_semaphore()
    for other in (left, right):
        pl.semaphore_signal(barrier, inc=1, device_id=(other, me_d), device_id_type=MESH)
    greeted = 2
    if scatter:
        for t in range(1, half):
            pl.semaphore_signal(barrier, inc=1, device_id=plane_device(t), device_id_type=MESH)
        for d in range(1, nd):
            @pl.when(me_d < d)
            def _(d=d):
                pl.semaphore_signal(barrier, inc=1, device_id=(me_l, d), device_id_type=MESH)
        greeted += half - 1 + me_d
    for c in load_w2:
        c.start()
    load_pre.start()
    load_inp.start()
    for c in load_w1:
        c.start()

    def halo_copies(send, recv, base):
        return [
            pltpu.make_async_remote_copy(
                src_ref=send.at[i], dst_ref=recv.at[i], send_sem=hs_sem.at[base],
                recv_sem=hr_sem.at[base], device_id=(other, me_d), device_id_type=MESH,
            )
            for i, other in enumerate((left, right))
        ]

    def pack(dst, src, start, width):
        for p in range(rows):
            dst[p * width : (p + 1) * width, :] = src[p, start : start + width, :]

    def side_inner(src, side, d):
        zero = jnp.zeros((rows, d, ch), BF16)
        side[:, cols - d : cols, 0:ch] = zero
        side[:, 0:d, ch : 2 * ch] = zero
        side[:, 0 : cols - d, 0:ch] = src[:, d:cols, :]
        side[:, d:cols, ch : 2 * ch] = src[:, 0 : cols - d, :]

    def side_fill(side, piece, lo_at, hi_at, width):
        side[:, lo_at : lo_at + width, 0:ch] = piece[0].reshape(rows, width, ch)
        side[:, hi_at : hi_at + width, ch : 2 * ch] = piece[1].reshape(rows, width, ch)

    def input_terms(src, at, lanes, w_v, wl, d, fresh):
        for r in (1, 0, 2):
            lo, hi, first = row_span(rows, d, r)
            term = dot_nt(
                flat(src[first : first + hi - lo, :, at : at + lanes]),
                w_v[r, :, wl : wl + lanes],
            )
            if fresh and r == 1:
                acc[...] = term
            else:
                acc[lo * cols : hi * cols, :] += term

    def scaled(value):
        return value if scatter else value * norm

    def weight_terms(x, src, at, lanes, dw, taps, d):
        for r in range(3):
            lo, hi, first = row_span(rows, d, r)
            term = dot_tn(flat(x[lo:hi]), flat(src[first : first + hi - lo, :, at : at + lanes]))
            for i, c in enumerate(taps):
                k = 3 * r + c
                dw[k * ch : (k + 1) * ch, :] = scaled(term[:, i * ch : (i + 1) * ch])

    def edge_terms(lo, hi, taps, width, parts, w_v):
        total = None
        for strip, slot in parts:
            for r, first in taps:
                term = dot_nt(
                    strip[first * width : (first + hi - lo) * width, :],
                    w_v[r, :, slot * ch : (slot + 1) * ch],
                )
                total = term if total is None else total + term
        return total

    if scatter:
        depth = dw1.shape[0] // (nl * nd)

        def owner(parity, d):
            total = 0
            for dd in range(nd):
                low, high = owners[0][dd], owners[1][dd]
                total = jnp.where(d == dd, low + parity * (high - low), total)
            return total

        def late(parity, d, i):
            return i + jnp.where(owner(parity, d) <= i, 1, 0)

        def chunk(dw, chip, d, parity, start, stop):
            at = pl.multiple_of(((2 * chip + parity) * nd + d) * depth, 8)
            return dw[pl.ds(at + start, stop - start), :]

        def remote(src, dst, send, recv, device):
            return pltpu.make_async_remote_copy(
                src_ref=src, dst_ref=dst, send_sem=send, recv_sem=recv,
                device_id=device, device_id_type=MESH,
            )

        def seen_from(chip):
            return lax.rem(my_chip - chip + half, half)

        sibling = (me_l + 1 - 2 * core, me_d)
        mine = owner(core, me_d)

        def early_pair(g, dw):
            b = banks[g]
            for d in range(nd):
                chip = owner(1 - core, d)
                b.ep_s[d] = chunk(dw, chip, d, 1 - core, 0, depth).astype(BF16)
            remote(b.ep_s, b.ep_r, b.ep_sem.at[0], b.ep_sem.at[1], sibling).start()

        def early_chip_sum(b, dw, d):
            return chunk(dw, owner(core, d), d, core, 0, depth) + b.ep_r[d].astype(F32)

        def early_depth(g, dw):
            b = banks[g]
            landed(b.ep_r, b.ep_sem.at[1])
            for u in range(1, nd):
                b.ez_s[u] = early_chip_sum(b, dw, lax.rem(me_d + u, nd)).astype(BF16)
                remote(
                    b.ez_s.at[u], b.ez_r.at[u], b.ez_sem.at[0], b.ez_sem.at[1], depth_device(u)
                ).start()

        def early_sum(b, dw):
            total = early_chip_sum(b, dw, me_d)
            for u in range(1, nd):
                total += b.ez_r[u].astype(F32)
            return total

        def early_plane(g, dw):
            b = banks[g]
            landed(b.ez_r.at[pl.ds(1, nd - 1)], b.ez_sem.at[1])

            @pl.when(my_chip != mine)
            def _():
                b.ex_s[...] = early_sum(b, dw).astype(BF16)
                remote(
                    b.ex_s, b.ex_r.at[seen_from(mine)], b.ex_sem.at[0], b.ex_sem.at[1],
                    (2 * mine + core, me_d),
                ).start()

        def late_pair(g, dw):
            b = banks[g]
            for i in range(half - 1):
                for d in range(nd):
                    chip = late(1 - core, d, i)
                    b.lp_s[i, d] = chunk(dw, chip, d, 1 - core, 0, depth).astype(BF16)
                remote(b.lp_s.at[i], b.lp_r.at[i], b.lps_sem, b.lpr_sem.at[i], sibling).start()

        def late_chip_sum(b, dw, chip, i, d, start, stop):
            return chunk(dw, chip, d, core, start, stop) + b.lp_r[i, d, start:stop, :].astype(F32)

        def late_first(g, dw):
            b = banks[g]
            for i in range(half - 1):
                landed(b.lp_r.at[i], b.lpr_sem.at[i])
                for d in range(nd):
                    chip = late(core, d, i)

                    @pl.when(chip != my_chip)
                    def _(i=i, d=d, chip=chip):
                        b.pa_s[d, i] = late_chip_sum(b, dw, chip, i, d, 0, b.pa_s.shape[2]).astype(BF16)
                        remote(
                            b.pa_s.at[d, i], b.pa_r.at[d, seen_from(chip)],
                            b.pas_sem.at[d], b.par_sem.at[d], (2 * chip + core, me_d),
                        ).start()
            for u in range(1, nd):
                d = lax.rem(me_d + u, nd)
                for i in range(half - 1):
                    chip = late(core, d, i)
                    b.za_s[u, i] = late_chip_sum(b, dw, chip, i, d, b.pa_s.shape[2], depth).astype(BF16)
                remote(
                    b.za_s.at[u], b.za_r.at[u], b.za_sem.at[0], b.za_sem.at[1], depth_device(u)
                ).start()

        def plane_sum(b, dw, d):
            i = my_chip - jnp.where(owner(core, d) < my_chip, 1, 0)
            total = late_chip_sum(b, dw, my_chip, i, d, 0, b.pa_s.shape[2])
            for t in range(1, half):
                total += b.pa_r[d, t].astype(F32)
            return total

        def depth_sum(b, dw, chip, i):
            total = late_chip_sum(b, dw, chip, i, me_d, b.pa_s.shape[2], depth)
            for u in range(1, nd):
                total += b.za_r[u, i].astype(F32)
            return total

        def late_second_plane(g, dw):
            b = banks[g]
            for u in (*range(1, nd), 0):
                d = lax.rem(me_d + u, nd)

                @pl.when(owner(core, d) != my_chip)
                def _(u=u, d=d):
                    landed(b.pa_r.at[d, pl.ds(1, half - 1)], b.par_sem.at[d])
                    if u:
                        b.pb_s[u] = plane_sum(b, dw, d).astype(BF16)
                        remote(
                            b.pb_s.at[u], b.pb_r.at[u], b.pbs_sem.at[u], b.pbr_sem,
                            depth_device(u),
                        ).start()

        def late_second_depth(g, dw):
            b = banks[g]
            landed(b.za_r.at[pl.ds(1, nd - 1)], b.za_sem.at[1])
            for i in range(half - 1):
                chip = late(core, me_d, i)

                @pl.when(chip != my_chip)
                def _(i=i, chip=chip):
                    b.zb_s[i] = depth_sum(b, dw, chip, i).astype(BF16)
                    remote(
                        b.zb_s.at[i], b.zb_r.at[seen_from(chip)],
                        b.zb_sem.at[0], b.zb_sem.at[1], (2 * chip + core, me_d),
                    ).start()

        def put(out, total, start, count):
            for i in range(2):
                out[pl.ds(2 * start + i, count, stride=2), :] = (
                    total[:, i * ch // 2 : (i + 1) * ch // 2] * norm
                )

        def last_stage(g, dw, out):
            b = banks[g]

            @pl.when(my_chip == mine)
            def _():
                total = early_sum(b, dw)
                landed(b.ex_r.at[pl.ds(1, half - 1)], b.ex_sem.at[1])
                for t in range(1, half):
                    total += b.ex_r[t].astype(F32)
                put(out, total, 0, depth)
                landed(b.zb_s, b.zb_sem.at[0])

            @pl.when(my_chip != mine)
            def _():
                landed(b.pb_r.at[pl.ds(1, nd - 1)], b.pbr_sem)
                total = plane_sum(b, dw, me_d)
                for u in range(1, nd):
                    total += b.pb_r[u].astype(F32)
                put(out, total, 0, b.pa_s.shape[2])
                landed(b.zb_r.at[pl.ds(1, half - 1)], b.zb_sem.at[1])
                total = depth_sum(b, dw, my_chip, my_chip - jnp.where(mine < my_chip, 1, 0))
                for t in range(1, half):
                    total += b.zb_r[t].astype(F32)
                put(out, total, b.pa_s.shape[2], depth - b.pa_s.shape[2])
                landed(b.zb_s.at[pl.ds(0, half - 2)], b.zb_sem.at[0])
                landed(b.ex_s, b.ex_sem.at[0])

            landed(b.ep_s, b.ep_sem.at[0])
            landed(b.ez_s.at[pl.ds(1, nd - 1)], b.ez_sem.at[0])
            landed(b.lp_s, b.lps_sem)
            landed(b.za_s.at[pl.ds(1, nd - 1)], b.za_sem.at[0])
            for u in range(nd):
                d = lax.rem(me_d + u, nd)

                @pl.when(owner(core, d) == my_chip)
                def _(d=d):
                    landed(b.pa_s.at[d], b.pas_sem.at[d])

                @pl.when(owner(core, d) != my_chip)
                def _(u=u, d=d):
                    landed(b.pa_s.at[d, pl.ds(0, half - 2)], b.pas_sem.at[d])
                    if u:
                        landed(b.pb_s.at[u], b.pbs_sem.at[u])

    load_cot.wait()
    pack(sa.at[0], cot_v, rest, first_d)
    pack(sa.at[1], cot_v, cols - second_d, first_d)
    pack(sb.at[0], cot_v, 0, rest)
    pack(sb.at[1], cot_v, cols - rest, rest)
    pl.semaphore_wait(barrier, greeted)
    if scatter:
        for d in range(nd - 1):
            @pl.when(me_d > d)
            def _(d=d):
                pl.semaphore_signal(greet, inc=1, device_id=(me_l, d), device_id_type=MESH)
    halo_a = halo_copies(sa, ra, 0)
    halo_b = halo_copies(sb, rb, 1)
    for c in halo_a + halo_b:
        c.start()

    outer = (cot_e, acc_e, first_d, (0, cols - first_d), (second_d, cols - first_d - second_d))
    inner = (
        cot_f, acc_f, rest, (first_d, cols - second_d),
        (first_d + second_d, cols - 2 * second_d),
    )

    def strip_packs(group):
        strips, _, width, own, other = group
        for e in range(2):
            pack(strips.at[e], cot_v, own[e], width)
            pack(strips.at[2 + e], cot_v, other[e], width)

    def strip_start(group):
        strips, sums_e, width, _, _ = group
        for e in range(2):
            for lo, hi, taps in row_blocks(rows, second_d):
                sums_e[e, lo * width : hi * width, :] = edge_terms(
                    lo, hi, taps, width, ((strips.at[e], 2), (strips.at[2 + e], e)), w2_v
                )

    def strip_finish(group, halo, pre_s, out):
        _, sums_e, width, _, _ = group
        for e in range(2):
            for lo, hi, taps in row_blocks(rows, second_d):
                part = slice(lo * width, hi * width)
                grad = sums_e[e, part, :] + edge_terms(
                    lo, hi, taps, width, ((halo.at[1 - e], 1 - e),), w2_v
                )
                out[e, part, :] = jnp.where(pre_s[e, part, :] > 0, grad, F32(0.0)).astype(BF16)

    def strip_place(group, value):
        _, _, width, own, _ = group
        for e in range(2):
            side1[:, own[e] : own[e] + width, 2 * ch : 3 * ch] = value[e].reshape(rows, width, ch)

    def edge_update(dw, d, groups):
        for r in range(3):
            lo, hi, first = row_span(rows, d, r)
            for e, c in ((1, 0), (0, 2)):
                total = None
                for own, halo, width in groups:
                    term = dot_tn(
                        own[e, lo * width : hi * width, :],
                        halo[1 - e, first * width : (first + hi - lo) * width, :],
                    )
                    total = term if total is None else total + term
                k = 3 * r + c
                dw[k * ch : (k + 1) * ch, :] += scaled(total)

    @section
    def _():
        side_inner(cot_v, side2, second_d)
        strip_packs(outer)
        strip_packs(inner)

    landed(w2_v, w2_sem)

    @section
    def _():
        strip_start(outer)

    load_pre.wait()

    @section
    def _():
        pre_v[...] = jnp.maximum(pre_v[...], jnp.zeros((), BF16))
        for e in range(2):
            pack(pre_e.at[e], pre_v, outer[3][e], first_d)
            pack(pre_f.at[e], pre_v, inner[3][e], rest)

    @section
    def _():
        input_terms(side2, 0, 3 * ch, w2_v, 0, second_d, True)

    @section
    def _():
        grad = jnp.where(flat(pre_v[...]) > 0, acc[...], F32(0.0)).astype(BF16)
        lg_v[...] = grad.reshape(rows, cols, ch)

    @section
    def _():
        weight_terms(pre_v, side2, 0, 3 * ch, dw2, (0, 2, 1), second_d)

    if scatter:
        early_pair(1, dw2)

    @section
    def _():
        strip_start(inner)

    landed(ra, hr_sem.at[0])

    @section
    def _():
        strip_finish(outer, ra, pre_e, sc)

    halo_c = halo_copies(sc, rc, 2)
    for c in halo_c:
        c.start()

    @section
    def _():
        strip_place(outer, sc)

    if scatter:
        @pl.when(me_d < nd - 1)
        def _():
            pl.semaphore_wait(greet, nd - 1 - me_d)

        early_depth(1, dw2)
    landed(rb, hr_sem.at[1])

    @section
    def _():
        strip_finish(inner, rb, pre_f, lg_f)
        strip_place(inner, lg_f)

    @section
    def _():
        edge_update(dw2, second_d, ((pre_e, ra, first_d), (pre_f, rb, rest)))

    if scatter:
        late_pair(1, dw2)
    load_inp.wait()

    @section
    def _():
        weight_terms(inp_v, side1, 2 * ch, ch, dw1, (1,), first_d)

    if scatter:
        early_pair(0, dw1)
    if scatter:
        late_first(1, dw2)

    @section
    def _():
        side_inner(lg_v, side1, first_d)
        pack(inp_e.at[0], inp_v, 0, first_d)
        pack(inp_e.at[1], inp_v, cols - first_d, first_d)

    @section
    def _():
        weight_terms(inp_v, side1, 0, 2 * ch, dw1, (0, 2), first_d)

    if scatter:
        early_depth(0, dw1)
    landed(rc, hr_sem.at[2])

    @section
    def _():
        edge_update(dw1, first_d, ((inp_e, rc, first_d),))

    if scatter:
        late_pair(0, dw1)

    @section
    def _():
        side_fill(side1, rc, cols - first_d, 0, first_d)

    landed(w1_v, w1_sem)
    if scatter:
        late_first(0, dw1)
    if scatter:
        early_plane(1, dw2)

    @section
    def _():
        input_terms(side1, 0, 3 * ch, w1_v, 0, first_d, True)
        ig_out[0] = acc[...].astype(BF16).reshape(rows, cols, ch)

    if scatter:
        late_second_plane(1, dw2)
    if scatter:
        late_second_depth(1, dw2)
    if scatter:
        late_second_plane(0, dw1)
    if scatter:
        late_second_depth(0, dw1)
    if scatter:
        early_plane(0, dw1)
    if scatter:
        last_stage(1, dw2, g2_out)
    if scatter:
        last_stage(0, dw1, g1_out)
    for i, ref in enumerate((sa, sb, sc)):
        landed(ref, hs_sem.at[i])


def emit_kernel(*refs):
    count = len(refs) // 2
    copies = [
        pltpu.make_async_copy(refs[i], refs[count + i], refs[-1].at[i]) for i in range(count)
    ]
    for c in copies:
        c.start()
    for c in copies:
        c.wait()


def emit(*values):
    any_spec = pl.BlockSpec(memory_space=pl.ANY)
    vmem_spec = pl.BlockSpec(memory_space=pltpu.VMEM)
    return pl.pallas_call(
        emit_kernel,
        out_shape=[jax.ShapeDtypeStruct(v.shape, v.dtype) for v in values],
        in_specs=[vmem_spec] * len(values),
        out_specs=[any_spec] * len(values),
        scratch_shapes=[pltpu.SemaphoreType.DMA((len(values),))],
        name="emit",
    )(*(pltpu.with_memory_space_constraint(v, pltpu.VMEM) for v in values))


def local(nl, nd, inputs, pre_act, cotangent, first_weight, second_weight):
    _, rows, cols, ch = inputs.shape
    taps_rows = first_weight.shape[0]
    norm = float(rows * cols * nl * inputs.shape[0] * nd) ** -0.5
    devices = nl * nd
    depth = taps_rows // devices
    even = nl % 2 == 0 and nl >= 6 and nd >= 2
    even = even and taps_rows % devices == 0 and depth % 8 == 0 and depth >= 16
    owners = early_owners(nl, nd, depth, ch) if even else None
    scatter = owners is not None
    vm = pltpu.VMEM
    dma = pltpu.SemaphoreType.DMA
    field = vm((rows, cols, ch), BF16)
    weights = vm((3, ch, 3 * ch), BF16)
    side = vm((rows, cols, 3 * ch), BF16)
    rest = SECOND_SPREAD - FIRST_SPREAD

    def strip(count, width, dtype=BF16):
        return vm((count, rows * width, ch), dtype)

    scratch = [field] * 2 + [weights] * 2 + [side] * 2 + [vm((rows * cols, ch), F32)]
    scratch += [strip(4, FIRST_SPREAD), strip(2, FIRST_SPREAD), strip(2, FIRST_SPREAD)]
    scratch += [strip(2, FIRST_SPREAD, F32)]
    scratch += [strip(4, rest), strip(2, rest), strip(2, rest, F32), strip(2, rest)]
    scratch += [dma((3,)), dma, dma]
    scratch += [strip(2, FIRST_SPREAD)] * 2 + [strip(2, rest)] * 2 + [strip(2, FIRST_SPREAD)] * 2
    scratch += [dma((3,)), dma((3,))]
    if scatter:
        scratch += [vm((taps_rows, ch), F32)] * 2
        for cut in first_rows(depth):
            scratch += bank_scratch(nl, nd, depth, ch, cut)
        scratch += [pltpu.SemaphoreType.REGULAR]
        grad_shape = (2 * depth, ch // 2)
    else:
        grad_shape = (taps_rows, ch)
    any_spec = pl.BlockSpec(memory_space=pl.ANY)
    vmem_spec = pl.BlockSpec(memory_space=pltpu.VMEM)
    place = vm if scatter else jax.ShapeDtypeStruct
    ig, g1, g2 = pl.pallas_call(
        functools.partial(kernel, nl, nd, owners, norm),
        out_shape=(
            place(inputs.shape, BF16),
            place(grad_shape, F32),
            place(grad_shape, F32),
        ),
        in_specs=[any_spec] * 5,
        out_specs=(vmem_spec, vmem_spec, vmem_spec),
        scratch_shapes=scratch,
        compiler_params=pltpu.CompilerParams(
            collective_id=0, has_side_effects=True, vmem_limit_bytes=62 * 1024 * 1024
        ),
        name="conv_backward",
    )(inputs, pre_act, cotangent, first_weight, second_weight)
    if scatter:
        ig, g1, g2 = emit(ig, g1, g2)
    g1, g2 = g1.reshape(-1), g2.reshape(-1)
    if not scatter:
        g1, g2 = (lax.psum_scatter(g, "lon", scatter_dimension=0, tiled=True) for g in (g1, g2))
        g1, g2 = (lax.psum_scatter(g, "dp", scatter_dimension=0, tiled=True) for g in (g1, g2))
    return ig, g1, g2


def solution(mesh):
    in_specs = (
        P("dp", None, "lon", None),
        P("dp", None, "lon", None),
        P("dp", None, "lon", None),
        P(),
        P(),
    )
    out_specs = (P("dp", None, "lon", None), P(("lon", "dp")), P(("lon", "dp")))
    step = functools.partial(local, mesh.shape["lon"], mesh.shape["dp"])
    return jax.shard_map(step, mesh=mesh, in_specs=in_specs, out_specs=out_specs, check_vma=False)
```

```python
import functools
import typing

import jax
import jax.numpy as jnp
from jax import lax
from jax.experimental import pallas as pl
from jax.experimental.pallas import tpu as pltpu
from jax.sharding import PartitionSpec as P

FIRST_SPREAD = 12
SECOND_SPREAD = 18
EMIT_PARTS = 4
MESH = pl.DeviceIdType.MESH
F32 = jnp.float32
BF16 = jnp.bfloat16
LANE_SLOT = (0, 2, 1)


def row_span(rows, dilation, r):
    if r == 0:
        return 0, rows - dilation, dilation
    if r == 1:
        return 0, rows, 0
    return dilation, rows, 0


class Bank(typing.NamedTuple):
    ep_s: typing.Any
    ep_r: typing.Any
    ez_s: typing.Any
    ez_r: typing.Any
    ex_s: typing.Any
    ex_r: typing.Any
    lp_s: typing.Any
    lp_r: typing.Any
    pa_s: typing.Any
    pa_r: typing.Any
    pb_s: typing.Any
    pb_r: typing.Any
    za_s: typing.Any
    za_r: typing.Any
    zb_s: typing.Any
    zb_r: typing.Any
    ep_sem: typing.Any
    ez_sem: typing.Any
    ex_sem: typing.Any
    lps_sem: typing.Any
    lpr_sem: typing.Any
    pas_sem: typing.Any
    par_sem: typing.Any
    pbs_sem: typing.Any
    pbr_sem: typing.Any
    za_sem: typing.Any
    zb_sem: typing.Any


def first_rows(depth):
    return depth * 8 // 72 * 8, depth * 7 // 72 * 8


def bank_scratch(nl, nd, depth, ch, cut):
    half = nl // 2
    dma = pltpu.SemaphoreType.DMA

    def buf(*shape):
        return pltpu.VMEM((*shape, ch), BF16)

    return [
        *[buf(nd, depth)] * 4, buf(depth), buf(half, depth),
        *[buf(half - 1, nd, depth)] * 2,
        buf(nd, half - 1, cut), buf(nd, half, cut), *[buf(nd, cut)] * 2,
        *[buf(nd, half - 1, depth - cut)] * 2, buf(half - 1, depth - cut), buf(half, depth - cut),
        dma((2,)), dma((2,)), dma((2,)), dma, dma((half - 1,)),
        dma((nd,)), dma((nd,)), dma((nd,)), dma, dma((2,)), dma((2,)),
    ]


def early_owners(nl, nd, depth, ch):
    table = []
    for parity in range(2):
        row = []
        for d in range(nd):
            chips = []
            for chip in range(nl // 2):
                start = ((2 * chip + parity) * nd + d) * depth
                taps = {start // ch % 3, (start + depth - 1) // ch % 3}
                if taps == {1} and depth <= ch:
                    chips.append(chip)
            if len(chips) != 1:
                return None
            row.append(chips[0])
        table.append(row)
    return table


def row_blocks(rows, dilation):
    cuts = sorted({0, dilation, rows - dilation, rows})
    blocks = []
    for lo, hi in zip(cuts, cuts[1:]):
        taps = []
        for r in range(3):
            start, stop, first = row_span(rows, dilation, r)
            if start <= lo and hi <= stop:
                taps.append((r, first + lo - start))
        blocks.append((lo, hi, taps))
    return blocks


def dot_nt(a, b):
    return lax.dot_general(a, b, (((1,), (1,)), ((), ())), preferred_element_type=F32)


def dot_tn(a, b):
    return lax.dot_general(a, b, (((0,), (0,)), ((), ())), preferred_element_type=F32)


def flat(v):
    return v.reshape(-1, v.shape[-1])


def kernel(nl, nd, owners, norm, *refs):
    refs = list(refs)
    scatter = owners is not None

    def take(count):
        taken = refs[:count]
        del refs[:count]
        return taken

    inp, pre, cot, w1, w2 = take(5)
    ig_out, g1_out, g2_out = take(3)
    pre_v, inp_v, w1_v, w2_v, side2, side1, acc = take(7)
    cot_e, pre_e, inp_e, acc_e, cot_f, pre_f, acc_f, lg_f = take(8)
    in_sem, w1_sem, w2_sem = take(3)
    sa, ra, sb, rb, sc, rc, hs_sem, hr_sem = take(8)
    if scatter:
        dw1, dw2 = take(2)
        banks = [Bank(*take(len(Bank._fields))) for _ in range(2)]
        (greet,) = take(1)
    else:
        dw1, dw2 = g1_out, g2_out

    rows, cols, ch = pre_v.shape
    first_d, second_d = FIRST_SPREAD, SECOND_SPREAD
    rest = second_d - first_d
    me_l, me_d = lax.axis_index("lon"), lax.axis_index("dp")
    left, right = lax.rem(me_l + nl - 1, nl), lax.rem(me_l + 1, nl)
    half = nl // 2
    core = lax.rem(me_l, 2)
    my_chip = me_l // 2
    cot_v = side2.at[:, :, pl.ds(2 * ch, ch)]
    lg_v = side1.at[:, :, pl.ds(2 * ch, ch)]
    section = pl.when(me_l >= 0)

    def plane_device(t):
        return (2 * lax.rem(my_chip + t, half) + core, me_d)

    def depth_device(u):
        return (me_l, lax.rem(me_d + u, nd))

    load_cot = pltpu.make_async_copy(cot.at[0], cot_v, in_sem.at[0])
    load_pre = pltpu.make_async_copy(pre.at[0], pre_v, in_sem.at[1])
    load_inp = pltpu.make_async_copy(inp.at[0], inp_v, in_sem.at[2])

    def weight_loads(w, w_v, sem):
        return [
            pltpu.make_async_copy(
                w.at[pl.ds(k * ch, ch)],
                w_v.at[k // 3, :, pl.ds(LANE_SLOT.index(k % 3) * ch, ch)],
                sem,
            )
            for k in range(9)
        ]

    load_w2 = weight_loads(w2, w2_v, w2_sem)
    load_w1 = weight_loads(w1, w1_v, w1_sem)

    def landed(ref, sem):
        pltpu.make_async_copy(ref, ref, sem).wait()

    load_cot.start()

    barrier = pltpu.get_barrier_semaphore()
    for other in (left, right):
        pl.semaphore_signal(barrier, inc=1, device_id=(other, me_d), device_id_type=MESH)
    greeted = 2
    if scatter:
        for t in range(1, half):
            pl.semaphore_signal(barrier, inc=1, device_id=plane_device(t), device_id_type=MESH)
        for d in range(1, nd):
            @pl.when(me_d < d)
            def _(d=d):
                pl.semaphore_signal(barrier, inc=1, device_id=(me_l, d), device_id_type=MESH)
        greeted += half - 1 + me_d
    for c in load_w2:
        c.start()
    load_pre.start()
    load_inp.start()
    for c in load_w1:
        c.start()

    def halo_copies(send, recv, base):
        return [
            pltpu.make_async_remote_copy(
                src_ref=send.at[i], dst_ref=recv.at[i], send_sem=hs_sem.at[base],
                recv_sem=hr_sem.at[base], device_id=(other, me_d), device_id_type=MESH,
            )
            for i, other in enumerate((left, right))
        ]

    def pack(dst, src, start, width):
        for p in range(rows):
            dst[p * width : (p + 1) * width, :] = src[p, start : start + width, :]

    def side_inner(src, side, d):
        zero = jnp.zeros((rows, d, ch), BF16)
        side[:, cols - d : cols, 0:ch] = zero
        side[:, 0:d, ch : 2 * ch] = zero
        side[:, 0 : cols - d, 0:ch] = src[:, d:cols, :]
        side[:, d:cols, ch : 2 * ch] = src[:, 0 : cols - d, :]

    def side_fill(side, piece, lo_at, hi_at, width):
        side[:, lo_at : lo_at + width, 0:ch] = piece[0].reshape(rows, width, ch)
        side[:, hi_at : hi_at + width, ch : 2 * ch] = piece[1].reshape(rows, width, ch)

    def input_terms(src, at, lanes, w_v, wl, d, fresh):
        for r in (1, 0, 2):
            lo, hi, first = row_span(rows, d, r)
            term = dot_nt(
                flat(src[first : first + hi - lo, :, at : at + lanes]),
                w_v[r, :, wl : wl + lanes],
            )
            if fresh and r == 1:
                acc[...] = term
            else:
                acc[lo * cols : hi * cols, :] += term

    def scaled(value):
        return value if scatter else value * norm

    def weight_terms(x, src, at, lanes, dw, taps, d):
        for r in range(3):
            lo, hi, first = row_span(rows, d, r)
            term = dot_tn(flat(x[lo:hi]), flat(src[first : first + hi - lo, :, at : at + lanes]))
            for i, c in enumerate(taps):
                k = 3 * r + c
                dw[k * ch : (k + 1) * ch, :] = scaled(term[:, i * ch : (i + 1) * ch])

    def edge_terms(lo, hi, taps, width, parts, w_v):
        total = None
        for strip, slot in parts:
            for r, first in taps:
                term = dot_nt(
                    strip[first * width : (first + hi - lo) * width, :],
                    w_v[r, :, slot * ch : (slot + 1) * ch],
                )
                total = term if total is None else total + term
        return total

    if scatter:
        depth = dw1.shape[0] // (nl * nd)

        def owner(parity, d):
            total = 0
            for dd in range(nd):
                low, high = owners[0][dd], owners[1][dd]
                total = jnp.where(d == dd, low + parity * (high - low), total)
            return total

        def late(parity, d, i):
            return i + jnp.where(owner(parity, d) <= i, 1, 0)

        def chunk(dw, chip, d, parity, start, stop):
            at = pl.multiple_of(((2 * chip + parity) * nd + d) * depth, 8)
            return dw[pl.ds(at + start, stop - start), :]

        def remote(src, dst, send, recv, device):
            return pltpu.make_async_remote_copy(
                src_ref=src, dst_ref=dst, send_sem=send, recv_sem=recv,
                device_id=device, device_id_type=MESH,
            )

        def seen_from(chip):
            return lax.rem(my_chip - chip + half, half)

        sibling = (me_l + 1 - 2 * core, me_d)
        mine = owner(core, me_d)

        def early_pair(g, dw):
            b = banks[g]
            for d in range(nd):
                chip = owner(1 - core, d)
                b.ep_s[d] = chunk(dw, chip, d, 1 - core, 0, depth).astype(BF16)
            remote(b.ep_s, b.ep_r, b.ep_sem.at[0], b.ep_sem.at[1], sibling).start()

        def early_chip_sum(b, dw, d):
            return chunk(dw, owner(core, d), d, core, 0, depth) + b.ep_r[d].astype(F32)

        def early_depth(g, dw):
            b = banks[g]
            landed(b.ep_r, b.ep_sem.at[1])
            for u in range(1, nd):
                b.ez_s[u] = early_chip_sum(b, dw, lax.rem(me_d + u, nd)).astype(BF16)
                remote(
                    b.ez_s.at[u], b.ez_r.at[u], b.ez_sem.at[0], b.ez_sem.at[1], depth_device(u)
                ).start()

        def early_sum(b, dw):
            total = early_chip_sum(b, dw, me_d)
            for u in range(1, nd):
                total += b.ez_r[u].astype(F32)
            return total

        def early_plane(g, dw):
            b = banks[g]
            landed(b.ez_r.at[pl.ds(1, nd - 1)], b.ez_sem.at[1])

            @pl.when(my_chip != mine)
            def _():
                b.ex_s[...] = early_sum(b, dw).astype(BF16)
                remote(
                    b.ex_s, b.ex_r.at[seen_from(mine)], b.ex_sem.at[0], b.ex_sem.at[1],
                    (2 * mine + core, me_d),
                ).start()

        def late_pair(g, dw):
            b = banks[g]
            for i in range(half - 1):
                for d in range(nd):
                    chip = late(1 - core, d, i)
                    b.lp_s[i, d] = chunk(dw, chip, d, 1 - core, 0, depth).astype(BF16)
                remote(b.lp_s.at[i], b.lp_r.at[i], b.lps_sem, b.lpr_sem.at[i], sibling).start()

        def late_chip_sum(b, dw, chip, i, d, start, stop):
            return chunk(dw, chip, d, core, start, stop) + b.lp_r[i, d, start:stop, :].astype(F32)

        def late_first(g, dw):
            b = banks[g]
            for i in range(half - 1):
                landed(b.lp_r.at[i], b.lpr_sem.at[i])
                for d in range(nd):
                    chip = late(core, d, i)

                    @pl.when(chip != my_chip)
                    def _(i=i, d=d, chip=chip):
                        b.pa_s[d, i] = late_chip_sum(b, dw, chip, i, d, 0, b.pa_s.shape[2]).astype(BF16)
                        remote(
                            b.pa_s.at[d, i], b.pa_r.at[d, seen_from(chip)],
                            b.pas_sem.at[d], b.par_sem.at[d], (2 * chip + core, me_d),
                        ).start()
            for u in range(1, nd):
                d = lax.rem(me_d + u, nd)
                for i in range(half - 1):
                    chip = late(core, d, i)
                    b.za_s[u, i] = late_chip_sum(b, dw, chip, i, d, b.pa_s.shape[2], depth).astype(BF16)
                remote(
                    b.za_s.at[u], b.za_r.at[u], b.za_sem.at[0], b.za_sem.at[1], depth_device(u)
                ).start()

        def plane_sum(b, dw, d):
            i = my_chip - jnp.where(owner(core, d) < my_chip, 1, 0)
            total = late_chip_sum(b, dw, my_chip, i, d, 0, b.pa_s.shape[2])
            for t in range(1, half):
                total += b.pa_r[d, t].astype(F32)
            return total

        def depth_sum(b, dw, chip, i):
            total = late_chip_sum(b, dw, chip, i, me_d, b.pa_s.shape[2], depth)
            for u in range(1, nd):
                total += b.za_r[u, i].astype(F32)
            return total

        def late_second_plane(g, dw):
            b = banks[g]
            for u in (*range(1, nd), 0):
                d = lax.rem(me_d + u, nd)

                @pl.when(owner(core, d) != my_chip)
                def _(u=u, d=d):
                    landed(b.pa_r.at[d, pl.ds(1, half - 1)], b.par_sem.at[d])
                    if u:
                        b.pb_s[u] = plane_sum(b, dw, d).astype(BF16)
                        remote(
                            b.pb_s.at[u], b.pb_r.at[u], b.pbs_sem.at[u], b.pbr_sem,
                            depth_device(u),
                        ).start()

        def late_second_depth(g, dw):
            b = banks[g]
            landed(b.za_r.at[pl.ds(1, nd - 1)], b.za_sem.at[1])
            for i in range(half - 1):
                chip = late(core, me_d, i)

                @pl.when(chip != my_chip)
                def _(i=i, chip=chip):
                    b.zb_s[i] = depth_sum(b, dw, chip, i).astype(BF16)
                    remote(
                        b.zb_s.at[i], b.zb_r.at[seen_from(chip)],
                        b.zb_sem.at[0], b.zb_sem.at[1], (2 * chip + core, me_d),
                    ).start()

        def put(out, total, start, count):
            for i in range(2):
                out[pl.ds(2 * start + i, count, stride=2), :] = (
                    total[:, i * ch // 2 : (i + 1) * ch // 2] * norm
                )

        def last_stage(g, dw, out):
            b = banks[g]

            @pl.when(my_chip == mine)
            def _():
                total = early_sum(b, dw)
                landed(b.ex_r.at[pl.ds(1, half - 1)], b.ex_sem.at[1])
                for t in range(1, half):
                    total += b.ex_r[t].astype(F32)
                put(out, total, 0, depth)
                landed(b.zb_s, b.zb_sem.at[0])

            @pl.when(my_chip != mine)
            def _():
                landed(b.pb_r.at[pl.ds(1, nd - 1)], b.pbr_sem)
                total = plane_sum(b, dw, me_d)
                for u in range(1, nd):
                    total += b.pb_r[u].astype(F32)
                put(out, total, 0, b.pa_s.shape[2])
                landed(b.zb_r.at[pl.ds(1, half - 1)], b.zb_sem.at[1])
                total = depth_sum(b, dw, my_chip, my_chip - jnp.where(mine < my_chip, 1, 0))
                for t in range(1, half):
                    total += b.zb_r[t].astype(F32)
                put(out, total, b.pa_s.shape[2], depth - b.pa_s.shape[2])
                landed(b.zb_s.at[pl.ds(0, half - 2)], b.zb_sem.at[0])
                landed(b.ex_s, b.ex_sem.at[0])

            landed(b.ep_s, b.ep_sem.at[0])
            landed(b.ez_s.at[pl.ds(1, nd - 1)], b.ez_sem.at[0])
            landed(b.lp_s, b.lps_sem)
            landed(b.za_s.at[pl.ds(1, nd - 1)], b.za_sem.at[0])
            for u in range(nd):
                d = lax.rem(me_d + u, nd)

                @pl.when(owner(core, d) == my_chip)
                def _(d=d):
                    landed(b.pa_s.at[d], b.pas_sem.at[d])

                @pl.when(owner(core, d) != my_chip)
                def _(u=u, d=d):
                    landed(b.pa_s.at[d, pl.ds(0, half - 2)], b.pas_sem.at[d])
                    if u:
                        landed(b.pb_s.at[u], b.pbs_sem.at[u])

    load_cot.wait()
    pack(sa.at[0], cot_v, rest, first_d)
    pack(sa.at[1], cot_v, cols - second_d, first_d)
    pl.semaphore_wait(barrier, greeted)
    if scatter:
        for d in range(nd - 1):
            @pl.when(me_d > d)
            def _(d=d):
                pl.semaphore_signal(greet, inc=1, device_id=(me_l, d), device_id_type=MESH)
    halo_a = halo_copies(sa, ra, 0)
    halo_b = halo_copies(sb, rb, 1)
    for c in halo_a:
        c.start()
    pack(sb.at[0], cot_v, 0, rest)
    pack(sb.at[1], cot_v, cols - rest, rest)
    for c in halo_b:
        c.start()

    outer = (cot_e, acc_e, first_d, (0, cols - first_d), (second_d, cols - first_d - second_d))
    inner = (
        cot_f, acc_f, rest, (first_d, cols - second_d),
        (first_d + second_d, cols - 2 * second_d),
    )

    def strip_packs(group):
        strips, _, width, own, other = group
        for e in range(2):
            pack(strips.at[e], cot_v, own[e], width)
            pack(strips.at[2 + e], cot_v, other[e], width)

    def strip_start(group):
        strips, sums_e, width, _, _ = group
        for e in range(2):
            for lo, hi, taps in row_blocks(rows, second_d):
                sums_e[e, lo * width : hi * width, :] = edge_terms(
                    lo, hi, taps, width, ((strips.at[e], 2), (strips.at[2 + e], e)), w2_v
                )

    def strip_finish(group, halo, pre_s, out):
        _, sums_e, width, _, _ = group
        for e in range(2):
            for lo, hi, taps in row_blocks(rows, second_d):
                part = slice(lo * width, hi * width)
                grad = sums_e[e, part, :] + edge_terms(
                    lo, hi, taps, width, ((halo.at[1 - e], 1 - e),), w2_v
                )
                out[e, part, :] = jnp.where(pre_s[e, part, :] > 0, grad, F32(0.0)).astype(BF16)

    def strip_place(group, value):
        _, _, width, own, _ = group
        for e in range(2):
            side1[:, own[e] : own[e] + width, 2 * ch : 3 * ch] = value[e].reshape(rows, width, ch)

    def edge_update(dw, d, groups):
        for r in range(3):
            lo, hi, first = row_span(rows, d, r)
            for e, c in ((1, 0), (0, 2)):
                total = None
                for own, halo, width in groups:
                    term = dot_tn(
                        own[e, lo * width : hi * width, :],
                        halo[1 - e, first * width : (first + hi - lo) * width, :],
                    )
                    total = term if total is None else total + term
                k = 3 * r + c
                dw[k * ch : (k + 1) * ch, :] += scaled(total)

    @section
    def _():
        side_inner(cot_v, side2, second_d)
        strip_packs(outer)
        strip_packs(inner)

    landed(w2_v, w2_sem)

    @section
    def _():
        strip_start(outer)

    load_pre.wait()

    @section
    def _():
        pre_v[...] = jnp.maximum(pre_v[...], jnp.zeros((), BF16))
        for e in range(2):
            pack(pre_e.at[e], pre_v, outer[3][e], first_d)
            pack(pre_f.at[e], pre_v, inner[3][e], rest)

    @section
    def _():
        input_terms(side2, 0, 3 * ch, w2_v, 0, second_d, True)

    @section
    def _():
        grad = jnp.where(flat(pre_v[...]) > 0, acc[...], F32(0.0)).astype(BF16)
        lg_v[...] = grad.reshape(rows, cols, ch)

    @section
    def _():
        weight_terms(pre_v, side2, 0, 3 * ch, dw2, (0, 2, 1), second_d)

    if scatter:
        early_pair(1, dw2)

    @section
    def _():
        strip_start(inner)

    landed(ra, hr_sem.at[0])

    @section
    def _():
        strip_finish(outer, ra, pre_e, sc)

    halo_c = halo_copies(sc, rc, 2)
    for c in halo_c:
        c.start()

    @section
    def _():
        strip_place(outer, sc)

    if scatter:
        @pl.when(me_d < nd - 1)
        def _():
            pl.semaphore_wait(greet, nd - 1 - me_d)

        early_depth(1, dw2)
    landed(rb, hr_sem.at[1])

    @section
    def _():
        strip_finish(inner, rb, pre_f, lg_f)
        strip_place(inner, lg_f)

    @section
    def _():
        edge_update(dw2, second_d, ((pre_e, ra, first_d), (pre_f, rb, rest)))

    if scatter:
        late_pair(1, dw2)
    load_inp.wait()

    @section
    def _():
        weight_terms(inp_v, side1, 2 * ch, ch, dw1, (1,), first_d)

    if scatter:
        early_pair(0, dw1)
    if scatter:
        late_first(1, dw2)

    @section
    def _():
        side_inner(lg_v, side1, first_d)
        pack(inp_e.at[0], inp_v, 0, first_d)
        pack(inp_e.at[1], inp_v, cols - first_d, first_d)

    @section
    def _():
        weight_terms(inp_v, side1, 0, 2 * ch, dw1, (0, 2), first_d)

    if scatter:
        early_depth(0, dw1)
    landed(rc, hr_sem.at[2])

    @section
    def _():
        edge_update(dw1, first_d, ((inp_e, rc, first_d),))

    if scatter:
        late_pair(0, dw1)

    @section
    def _():
        side_fill(side1, rc, cols - first_d, 0, first_d)

    landed(w1_v, w1_sem)
    if scatter:
        late_first(0, dw1)
    if scatter:
        early_plane(1, dw2)

    @section
    def _():
        input_terms(side1, 0, 3 * ch, w1_v, 0, first_d, True)
        ig_out[0] = acc[...].astype(BF16).reshape(rows, cols, ch)

    if scatter:
        late_second_plane(1, dw2)
    if scatter:
        late_second_depth(1, dw2)
    if scatter:
        late_second_plane(0, dw1)
    if scatter:
        late_second_depth(0, dw1)
    if scatter:
        early_plane(0, dw1)
    if scatter:
        last_stage(1, dw2, g2_out)
    if scatter:
        last_stage(0, dw1, g1_out)
    for i, ref in enumerate((sa, sb, sc)):
        landed(ref, hs_sem.at[i])


def emit_kernel(*refs):
    count = len(refs) // 2
    sem = refs[-1]
    for i in range(count):
        src, dst = refs[i], refs[count + i]
        if src.ndim == 4 and src.shape[1] % EMIT_PARTS == 0:
            rows = src.shape[1] // EMIT_PARTS
            for q in range(EMIT_PARTS):
                part = pl.ds(q * rows, rows)
                pltpu.make_async_copy(src.at[:, part], dst.at[:, part], sem.at[i]).start()
        else:
            pltpu.make_async_copy(src, dst, sem.at[i]).start()
    for i in range(count):
        pltpu.make_async_copy(refs[i], refs[count + i], sem.at[i]).wait()


def emit(*values):
    any_spec = pl.BlockSpec(memory_space=pl.ANY)
    vmem_spec = pl.BlockSpec(memory_space=pltpu.VMEM)
    return pl.pallas_call(
        emit_kernel,
        out_shape=[jax.ShapeDtypeStruct(v.shape, v.dtype) for v in values],
        in_specs=[vmem_spec] * len(values),
        out_specs=[any_spec] * len(values),
        scratch_shapes=[pltpu.SemaphoreType.DMA((len(values),))],
        name="emit",
    )(*(pltpu.with_memory_space_constraint(v, pltpu.VMEM) for v in values))


def local(nl, nd, inputs, pre_act, cotangent, first_weight, second_weight):
    _, rows, cols, ch = inputs.shape
    taps_rows = first_weight.shape[0]
    norm = float(rows * cols * nl * inputs.shape[0] * nd) ** -0.5
    devices = nl * nd
    depth = taps_rows // devices
    even = nl % 2 == 0 and nl >= 6 and nd >= 2
    even = even and taps_rows % devices == 0 and depth % 8 == 0 and depth >= 16
    owners = early_owners(nl, nd, depth, ch) if even else None
    scatter = owners is not None
    vm = pltpu.VMEM
    dma = pltpu.SemaphoreType.DMA
    field = vm((rows, cols, ch), BF16)
    weights = vm((3, ch, 3 * ch), BF16)
    side = vm((rows, cols, 3 * ch), BF16)
    rest = SECOND_SPREAD - FIRST_SPREAD

    def strip(count, width, dtype=BF16):
        return vm((count, rows * width, ch), dtype)

    scratch = [field] * 2 + [weights] * 2 + [side] * 2 + [vm((rows * cols, ch), F32)]
    scratch += [strip(4, FIRST_SPREAD), strip(2, FIRST_SPREAD), strip(2, FIRST_SPREAD)]
    scratch += [strip(2, FIRST_SPREAD, F32)]
    scratch += [strip(4, rest), strip(2, rest), strip(2, rest, F32), strip(2, rest)]
    scratch += [dma((3,)), dma, dma]
    scratch += [strip(2, FIRST_SPREAD)] * 2 + [strip(2, rest)] * 2 + [strip(2, FIRST_SPREAD)] * 2
    scratch += [dma((3,)), dma((3,))]
    if scatter:
        scratch += [vm((taps_rows, ch), F32)] * 2
        for cut in first_rows(depth):
            scratch += bank_scratch(nl, nd, depth, ch, cut)
        scratch += [pltpu.SemaphoreType.REGULAR]
        grad_shape = (2 * depth, ch // 2)
    else:
        grad_shape = (taps_rows, ch)
    any_spec = pl.BlockSpec(memory_space=pl.ANY)
    vmem_spec = pl.BlockSpec(memory_space=pltpu.VMEM)
    place = vm if scatter else jax.ShapeDtypeStruct
    ig, g1, g2 = pl.pallas_call(
        functools.partial(kernel, nl, nd, owners, norm),
        out_shape=(
            place(inputs.shape, BF16),
            place(grad_shape, F32),
            place(grad_shape, F32),
        ),
        in_specs=[any_spec] * 5,
        out_specs=(vmem_spec, vmem_spec, vmem_spec),
        scratch_shapes=scratch,
        compiler_params=pltpu.CompilerParams(
            collective_id=0, has_side_effects=True, vmem_limit_bytes=62 * 1024 * 1024
        ),
        name="conv_backward",
    )(inputs, pre_act, cotangent, first_weight, second_weight)
    if scatter:
        ig, g1, g2 = emit(ig, g1, g2)
    g1, g2 = g1.reshape(-1), g2.reshape(-1)
    if not scatter:
        g1, g2 = (lax.psum_scatter(g, "lon", scatter_dimension=0, tiled=True) for g in (g1, g2))
        g1, g2 = (lax.psum_scatter(g, "dp", scatter_dimension=0, tiled=True) for g in (g1, g2))
    return ig, g1, g2


def solution(mesh):
    in_specs = (
        P("dp", None, "lon", None),
        P("dp", None, "lon", None),
        P("dp", None, "lon", None),
        P(),
        P(),
    )
    out_specs = (P("dp", None, "lon", None), P(("lon", "dp")), P(("lon", "dp")))
    step = functools.partial(local, mesh.shape["lon"], mesh.shape["dp"])
    return jax.shard_map(step, mesh=mesh, in_specs=in_specs, out_specs=out_specs, check_vma=False)
```
